32 devices in a mesh: row: 16 (over z, x, core), col: 2 (over y).
Axes of the slice: x: 2, y: 2, z: 4, core: 2. Of those that a mesh axis runs over, the one named last changes fastest.
Arguments:
- pair_map: float32 [256, 256, 128], P('row', 'col'), may hold values from -6 to 6
- pair_mask: int32 [256, 256], P('row', 'col'), may hold values 0 or 1
- in_gain: float32 [128], replicated, may hold values from 0.25 to 1.75
- in_bias: float32 [128], replicated, may hold values from -3 to 3
- w_proj: bfloat16 [128, 512], replicated, may hold values from -0.5 to 0.5
- w_gate: bfloat16 [128, 128], replicated, may hold values from -0.5 to 0.5
- out_gain: float32 [128], replicated, may hold values from 0.25 to 1.75
- out_bias: float32 [128], replicated, may hold values from -3 to 3
- w_out: bfloat16 [128, 128], replicated, may hold values from -0.5 to 0.5
Outputs:
- update: float32 [256, 256, 128], P('row', 'col')
The draws below stay inside these ranges and needn't reach their ends.
All inputs are finite; a program needn't handle non-finite values. No bound on the sum of `pair_mask` on one device may be relied on, other than what follows from the above.
Results may differ from the reference program's by a relative error of at most 0.0035.
Values may be sent and summed in bfloat16 or wider, within the bound.
No kernel may reach another device: no remote copies, remote signals or barrier semaphores. Data moves between devices by JAX's collectives and lax.ppermute only.
A program may use at most 128 MiB of HBM per device.

```python
import jax
import jax.numpy as jnp
from jax import lax

C = 128
CH = 128
NRES = 256


def place_ends(drawn, key, least, top_value):
    shape = drawn.shape
    index_at = [jax.random.randint(jax.random.fold_in(key, axis), (), 0, shape[axis]) for axis in range(len(shape))]
    drawn = drawn.at[tuple(index_at)].set(least)
    longest = shape.index(max(shape))
    index_at[longest] = (index_at[longest] + 1) % shape[longest]
    return drawn.at[tuple(index_at)].set(top_value)


def block_levels(own_key, dims, shards, low, top_value):
    level = 1.0
    for axis_at, parts in shards:
        draws = jax.random.uniform(jax.random.fold_in(jax.random.fold_in(own_key, 6), axis_at), (parts,), jnp.float32, low / len(shards), top_value / len(shards))
        level = level * jnp.repeat(jnp.exp(draws), dims[axis_at] // parts).reshape((-1,) + (1,) * (len(dims) - 1 - axis_at))
    return level


def noise(own_key, extent, deviation, reach, pieces=(), held_as=jnp.bfloat16):
    loudness = block_levels(own_key, extent, pieces, -0.22, 0.18) if pieces else 1.0
    entries = jax.random.normal(own_key, extent, jnp.float32) * deviation * loudness
    return jnp.minimum(jnp.maximum(entries, -reach), reach).astype(held_as)


def setup_inputs(seed: int = 0) -> dict:
    streams_of = jax.random.split(jax.random.key(seed), 10)
    return {
        "pair_map": noise(streams_of[0], (NRES, NRES, C), 1.0, 6.0, ((0, 16), (1, 2)), jnp.float32),
        "pair_mask": place_ends((jax.random.randint(streams_of[1], (NRES, NRES), 0, 4) < 3).astype(jnp.int32), jax.random.fold_in(streams_of[1], 1), 0, 1),
        "in_gain": jnp.clip(1.0 + 0.15 * jax.random.normal(streams_of[2], (C,), jnp.float32), 0.25, 1.75),
        "in_bias": noise(streams_of[3], (C,), 0.5, 3.0, (), jnp.float32),
        "w_proj": noise(streams_of[4], (C, 4 * CH), C ** -0.5, 0.5),
        "w_gate": noise(streams_of[5], (C, C), C ** -0.5, 0.5),
        "out_gain": jnp.clip(1.0 + 0.15 * jax.random.normal(streams_of[6], (CH,), jnp.float32), 0.25, 1.75),
        "out_bias": noise(streams_of[7], (CH,), 0.5, 3.0, (), jnp.float32),
        "w_out": noise(streams_of[8], (CH, C), CH ** -0.5, 0.5),
    }


def layer_norm(values, gain, bias):
    average = lax.optimization_barrier(jnp.mean(values, axis=-1, keepdims=True))
    variance = lax.optimization_barrier(jnp.mean(jnp.square(values - average), axis=-1, keepdims=True))
    return (values - average) * lax.rsqrt(variance + 1e-05) * gain + bias

def reference(pair_map, pair_mask, in_gain, in_bias, w_proj, w_gate, out_gain, out_bias, w_out):
    normed = layer_norm(pair_map, in_gain, in_bias).astype(jnp.bfloat16)
    flattened = normed.reshape(-1, C)
    projected = jnp.dot(flattened, w_proj, preferred_element_type=jnp.float32).reshape(NRES, NRES, 4 * CH)
    masked = pair_mask.astype(jnp.float32)[..., None]
    left_side = (masked * jax.nn.sigmoid(projected[..., :CH]) * projected[..., CH:2 * CH]).astype(jnp.bfloat16)
    right_side = (masked * jax.nn.sigmoid(projected[..., 2 * CH:3 * CH]) * projected[..., 3 * CH:]).astype(jnp.bfloat16)
    gating = jax.nn.sigmoid(jnp.dot(flattened, w_gate, preferred_element_type=jnp.float32)).reshape(NRES, NRES, C)
    summed = jnp.einsum('ikc,jkc->ijc', left_side.astype(jnp.float32), right_side.astype(jnp.float32), precision=lax.Precision.HIGHEST)
    normed_sum = layer_norm(summed, out_gain, out_bias).astype(jnp.bfloat16)
    result = jnp.dot(normed_sum.reshape(-1, CH), w_out, preferred_element_type=jnp.float32).reshape(NRES, NRES, C)
    return gating * result
```

```python
import functools

import jax
import jax.numpy as jnp
from jax import lax
from jax.experimental import pallas as pl
from jax.experimental.pallas import tpu as pltpu
from jax.sharding import PartitionSpec as P

F32 = jnp.float32
BF16 = jnp.bfloat16
EPSILON = 1e-05
NT = (((1,), (1,)), ((), ()))


def layer_norm(values, gain, bias):
    average = jnp.mean(values, axis=-1, keepdims=True)
    variance = jnp.mean(jnp.square(values - average), axis=-1, keepdims=True)
    return (values - average) * lax.rsqrt(variance + EPSILON) * gain + bias


def gathered(pair_map, pair_mask, in_gain, in_bias, w_proj, w_gate, out_gain, out_bias, w_out):
    row_count, col_count, channels = pair_map.shape
    hidden_width = w_out.shape[0]
    normed_map = layer_norm(pair_map, in_gain, in_bias).astype(BF16)
    flattened = normed_map.reshape(-1, channels)
    projected_all = jnp.dot(flattened, w_proj, preferred_element_type=F32).reshape(
        row_count, col_count, 4 * hidden_width
    )
    masked = pair_mask.astype(F32)[..., None]
    left_side = (
        masked
        * jax.nn.sigmoid(projected_all[..., :hidden_width])
        * projected_all[..., hidden_width : 2 * hidden_width]
    ).astype(BF16)
    gating = jax.nn.sigmoid(jnp.dot(flattened, w_gate, preferred_element_type=F32)).reshape(
        row_count, col_count, channels
    )
    right_side = (
        masked
        * jax.nn.sigmoid(projected_all[..., 2 * hidden_width : 3 * hidden_width])
        * projected_all[..., 3 * hidden_width :]
    ).astype(BF16)
    partial_value = jnp.einsum(
        "ikc,jkc->ijc",
        left_side,
        lax.all_gather(right_side, "row", axis=0, tiled=True),
        preferred_element_type=F32,
    )
    summed = lax.psum_scatter(partial_value, "col", scatter_dimension=1, tiled=True)
    normed_sum = layer_norm(summed, out_gain, out_bias).astype(BF16)
    result = jnp.dot(normed_sum.reshape(-1, hidden_width), w_out, preferred_element_type=F32).reshape(
        row_count, col_count, channels
    )
    return gating * result


def project_kernel(map_ref, mask_ref, gain_ref, bias_ref, w_proj_ref, w_gate_ref, sides_ref, gating_ref, w_scr, side_scr):
    step = pl.program_id(0)
    block, cols, channels = map_ref.shape
    hidden = w_proj_ref.shape[1] // 4
    rows = mask_ref.shape[0]

    @pl.when(step == 0)
    def _():
        for part in range(4):
            columns = w_proj_ref[:, part * hidden : (part + 1) * hidden]
            w_scr[part * hidden : (part + 1) * hidden, :] = columns.astype(F32).T.astype(BF16)

    values = map_ref[...].reshape(block * cols, channels)
    normed = layer_norm(values, gain_ref[...], bias_ref[...]).astype(BF16)
    gates = jax.nn.sigmoid(jnp.dot(normed, w_gate_ref[...], preferred_element_type=F32))
    gating_ref[...] = gates.reshape(block, cols, channels)
    projected = lax.dot_general(w_scr[...], normed, NT, preferred_element_type=F32)
    for at in range(block):
        row = step * block + at
        masked = mask_ref[pl.ds(row, 1), :].astype(F32)
        here = projected[:, at * cols : (at + 1) * cols]
        for side in range(2):
            gate = here[2 * side * hidden : (2 * side + 1) * hidden]
            value = here[(2 * side + 1) * hidden : (2 * side + 2) * hidden]
            side_scr[side, pl.ds(row, hidden, stride=rows), :] = masked * jax.nn.sigmoid(gate) * value

    @pl.when(step == pl.num_programs(0) - 1)
    def _():
        parts, _, share = sides_ref.shape[:3]
        for side in range(2):
            sides_ref[:, side] = side_scr[side].astype(BF16).reshape(parts, share, rows, cols)


def pairs_kernel(sides_ref, out_ref):
    row_parts, col_parts, _, _, rows, cols = sides_ref.shape

    def side(which):
        return jnp.concatenate(
            [sides_ref[:, q, which, 0].reshape(row_parts * rows, cols) for q in range(col_parts)], axis=1
        )

    summed = lax.dot_general(side(0), side(1), NT, preferred_element_type=F32).astype(BF16)
    for q in range(col_parts):
        out_ref[:, q, 0] = summed[:, q * cols : (q + 1) * cols].reshape(row_parts, rows, cols)


def output_kernel(summed_ref, gating_ref, gain_ref, bias_ref, w_out_ref, out_ref, scr):
    step = pl.program_id(0)
    hidden, rows, cols = summed_ref.shape
    block, _, channels = out_ref.shape

    @pl.when(step == 0)
    def _():
        values = summed_ref[...].astype(F32)
        average = jnp.sum(values, axis=0, keepdims=True) / hidden
        centred = values - average
        variance = jnp.sum(jnp.square(centred), axis=0, keepdims=True) / hidden
        scr[...] = (centred * lax.rsqrt(variance + EPSILON)).reshape(hidden * rows, cols)

    for at in range(block):
        scaled = scr[pl.ds(step * block + at, hidden, stride=rows), :].T
        normed_sum = (scaled * gain_ref[...] + bias_ref[...]).astype(BF16)
        result = jnp.dot(normed_sum, w_out_ref[...], preferred_element_type=F32)
        out_ref[at] = gating_ref[at] * result


def whole(shape):
    return pl.BlockSpec(shape, lambda *_: (0,) * len(shape))


def exchanged(
    pair_map, pair_mask, in_gain, in_bias, w_proj, w_gate, out_gain, out_bias, w_out, *, row_parts, col_parts
):
    rows, cols, channels = pair_map.shape
    hidden = w_out.shape[0]
    parts = row_parts * col_parts
    share = hidden // parts
    block = 4
    sides, gating = pl.pallas_call(
        project_kernel,
        grid=(rows // block,),
        in_specs=[
            pl.BlockSpec((block, cols, channels), lambda i: (i, 0, 0)),
            whole((rows, cols)),
            whole((1, channels)),
            whole((1, channels)),
            whole(w_proj.shape),
            whole(w_gate.shape),
        ],
        out_specs=[
            whole((parts, 2, share, rows, cols)),
            pl.BlockSpec((block, cols, channels), lambda i: (i, 0, 0)),
        ],
        out_shape=[
            jax.ShapeDtypeStruct((parts, 2, share, rows, cols), BF16),
            jax.ShapeDtypeStruct((rows, cols, channels), F32),
        ],
        scratch_shapes=[
            pltpu.VMEM((4 * hidden, channels), BF16),
            pltpu.VMEM((2, hidden * rows, cols), F32),
        ],
        name="project",
    )(pair_map, pair_mask, in_gain.reshape(1, -1), in_bias.reshape(1, -1), w_proj, w_gate)
    sides = lax.all_to_all(sides, ("row", "col"), 0, 0, tiled=True)
    sides = sides.reshape(row_parts, col_parts, 2, share, rows, cols)
    summed = pl.pallas_call(
        pairs_kernel,
        grid=(share,),
        in_specs=[pl.BlockSpec((row_parts, col_parts, 2, 1, rows, cols), lambda c: (0, 0, 0, c, 0, 0))],
        out_specs=pl.BlockSpec((row_parts, col_parts, 1, rows, cols), lambda c: (0, 0, c, 0, 0)),
        out_shape=jax.ShapeDtypeStruct((row_parts, col_parts, share, rows, cols), BF16),
        name="pairs",
    )(sides)
    summed = summed.reshape(parts, share, rows, cols)
    summed = lax.all_to_all(summed, ("row", "col"), 0, 0, tiled=True).reshape(hidden, rows, cols)
    return pl.pallas_call(
        output_kernel,
        grid=(rows // block,),
        in_specs=[
            whole((hidden, rows, cols)),
            pl.BlockSpec((block, cols, channels), lambda i: (i, 0, 0)),
            whole((1, hidden)),
            whole((1, hidden)),
            whole(w_out.shape),
        ],
        out_specs=pl.BlockSpec((block, cols, channels), lambda i: (i, 0, 0)),
        out_shape=jax.ShapeDtypeStruct((rows, cols, channels), F32),
        scratch_shapes=[pltpu.VMEM((hidden * rows, cols), F32)],
        name="output",
    )(summed, gating, out_gain.reshape(1, -1), out_bias.reshape(1, -1), w_out)


def solution(mesh):
    row_parts, col_parts = mesh.shape["row"], mesh.shape["col"]

    def local(pair_map, pair_mask, in_gain, in_bias, w_proj, w_gate, out_gain, out_bias, w_out):
        rows, cols, channels = pair_map.shape
        hidden = w_out.shape[0]
        whole_tiles = rows % 16 == 0 and cols % 128 == 0 and channels % 128 == 0 and hidden % 128 == 0
        plan = gathered
        if whole_tiles and hidden % (row_parts * col_parts) == 0:
            plan = functools.partial(exchanged, row_parts=row_parts, col_parts=col_parts)
        return plan(pair_map, pair_mask, in_gain, in_bias, w_proj, w_gate, out_gain, out_bias, w_out)

    in_specs = (P("row", "col", None), P("row", "col"), P(), P(), P(), P(), P(), P(), P())
    out_specs = P("row", "col", None)
    return jax.shard_map(local, mesh=mesh, in_specs=in_specs, out_specs=out_specs, check_vma=False)
```

```python
import functools

import jax
import jax.numpy as jnp
from jax import lax
from jax.experimental import pallas as pl
from jax.experimental.pallas import tpu as pltpu
from jax.sharding import PartitionSpec as P

F32 = jnp.float32
BF16 = jnp.bfloat16
EPSILON = 1e-05
NT = (((1,), (1,)), ((), ()))


def layer_norm(values, gain, bias):
    average = jnp.mean(values, axis=-1, keepdims=True)
    variance = jnp.mean(jnp.square(values - average), axis=-1, keepdims=True)
    return (values - average) * lax.rsqrt(variance + EPSILON) * gain + bias


def gathered(pair_map, pair_mask, in_gain, in_bias, w_proj, w_gate, out_gain, out_bias, w_out):
    row_count, col_count, channels = pair_map.shape
    hidden_width = w_out.shape[0]
    normed_map = layer_norm(pair_map, in_gain, in_bias).astype(BF16)
    flattened = normed_map.reshape(-1, channels)
    projected_all = jnp.dot(flattened, w_proj, preferred_element_type=F32).reshape(
        row_count, col_count, 4 * hidden_width
    )
    masked = pair_mask.astype(F32)[..., None]
    left_side = (
        masked
        * jax.nn.sigmoid(projected_all[..., :hidden_width])
        * projected_all[..., hidden_width : 2 * hidden_width]
    ).astype(BF16)
    gating = jax.nn.sigmoid(jnp.dot(flattened, w_gate, preferred_element_type=F32)).reshape(
        row_count, col_count, channels
    )
    right_side = (
        masked
        * jax.nn.sigmoid(projected_all[..., 2 * hidden_width : 3 * hidden_width])
        * projected_all[..., 3 * hidden_width :]
    ).astype(BF16)
    partial_value = jnp.einsum(
        "ikc,jkc->ijc",
        left_side,
        lax.all_gather(right_side, "row", axis=0, tiled=True),
        preferred_element_type=F32,
    )
    summed = lax.psum_scatter(partial_value, "col", scatter_dimension=1, tiled=True)
    normed_sum = layer_norm(summed, out_gain, out_bias).astype(BF16)
    result = jnp.dot(normed_sum.reshape(-1, hidden_width), w_out, preferred_element_type=F32).reshape(
        row_count, col_count, channels
    )
    return gating * result


HALVES = 2
VMEM_LIMIT = 16 * 2**20
HBM = pl.BlockSpec(memory_space=pltpu.MemorySpace.HBM)
VMEM = pl.BlockSpec(memory_space=pltpu.MemorySpace.VMEM)


def gated(gate, value):
    half = 0.5 * value
    return half * jnp.tanh(0.5 * gate) + half


def in_hbm(array):
    return pltpu.with_memory_space_constraint(array, pltpu.MemorySpace.HBM)


def own_place(row_groups, col_parts):
    row, col = lax.axis_index("row"), lax.axis_index("col")
    return lax.rem(row, row_groups), col


def start_copies(pairs, semaphores):
    copies = [pltpu.make_async_copy(source, target, semaphores.at[n]) for n, (source, target) in enumerate(pairs)]
    for copy in copies:
        copy.start()
    return [copy.wait for copy in copies]


def project(map_scr, mask_scr, gain_scr, bias_scr, w_scr, w_turned, side_scr, waits, extra):
    rows, cols, channels = map_scr.shape
    hidden = w_scr.shape[1] // 2
    wait_mask, wait_gain, wait_bias, wait_w, *wait_blocks = waits
    wait_w()
    for part in range(2):
        columns = w_scr[:, part * hidden : (part + 1) * hidden]
        w_turned[part * hidden : (part + 1) * hidden, :] = columns.astype(F32).T.astype(BF16)
    wait_gain()
    wait_bias()
    wait_mask()
    block = rows // len(wait_blocks)
    for step, wait_block in enumerate(wait_blocks):
        wait_block()
        values = map_scr[step * block : (step + 1) * block].reshape(block * cols, channels)
        normed = layer_norm(values, gain_scr[...], bias_scr[...]).astype(BF16)
        projected = lax.dot_general(w_turned[...], normed, NT, preferred_element_type=F32)
        for at in range(block):
            row = step * block + at
            here = projected[:, at * cols : (at + 1) * cols]
            masked = mask_scr[row : row + 1, :].astype(F32)
            side_scr[pl.ds(row, hidden, stride=rows), :] = masked * gated(here[:hidden], here[hidden:])
        if extra is not None:
            extra(step * block, block, normed)


def right_kernel(map_hbm, mask_hbm, gain_hbm, bias_hbm, w_hbm, out_ref, map_scr, mask_scr, gain_scr, bias_scr, w_scr, w_turned, side_scr, sems):
    rows = map_scr.shape[0]
    halves, groups, share, _, cols = out_ref.shape
    width = w_scr.shape[1]
    block = rows // 4
    waits = start_copies(
        [
            (mask_hbm, mask_scr),
            (gain_hbm, gain_scr),
            (bias_hbm, bias_scr),
            (w_hbm.at[:, width : 2 * width], w_scr),
        ]
        + [(map_hbm.at[pl.ds(n * block, block)], map_scr.at[pl.ds(n * block, block)]) for n in range(4)],
        sems,
    )
    project(map_scr, mask_scr, gain_scr, bias_scr, w_scr, w_turned, side_scr, waits, None)
    for group in range(groups):
        side = side_scr[group * share * rows : (group + 1) * share * rows].astype(BF16).reshape(share, rows, cols)
        for half in range(halves):
            out_ref[half, group] = side


def left_kernel(map_hbm, mask_hbm, gain_hbm, bias_hbm, w_hbm, w_gate_hbm, *refs, groups, row_groups, col_parts):
    outs, gating_ref = refs[:groups], refs[groups]
    map_scr, mask_scr, gain_scr, bias_scr, w_scr, w_turned, side_scr, w_gate_scr, sems = refs[groups + 1 :]
    rows = map_scr.shape[0]
    share, _, cols = outs[0].shape
    width = w_scr.shape[1]
    block = rows // 4
    wait_gate, *waits = start_copies(
        [
            (w_gate_hbm, w_gate_scr),
            (mask_hbm, mask_scr),
            (gain_hbm, gain_scr),
            (bias_hbm, bias_scr),
            (w_hbm.at[:, :width], w_scr),
        ]
        + [(map_hbm.at[pl.ds(n * block, block)], map_scr.at[pl.ds(n * block, block)]) for n in range(4)],
        sems,
    )
    wait_gate()

    def gate(first, count, normed):
        gates = jnp.dot(normed, w_gate_scr[...], preferred_element_type=F32)
        gating_ref[first : first + count] = gated(gates, jnp.ones_like(gates)).reshape(count, cols, -1)

    project(map_scr, mask_scr, gain_scr, bias_scr, w_scr, w_turned, side_scr, waits, gate)
    row, col = own_place(row_groups, col_parts)
    own = row * col_parts + col
    for offset, out_ref in enumerate(outs):
        start = pl.multiple_of((own ^ offset) * (share * rows), share * rows)
        out_ref[...] = side_scr[pl.ds(start, share * rows), :].astype(BF16).reshape(share, rows, cols)


def pairs_kernel(right_ref, *refs, row_groups, col_parts):
    lefts, out_ref = refs[:-1], refs[-1]
    row_parts, _, share, rows, cols = right_ref.shape
    row, col = own_place(row_groups, col_parts)
    for c in range(share):
        left = jnp.concatenate(
            [
                jnp.concatenate([lefts[at * col_parts + q][c] for at in range(row_groups)], axis=0)
                for q in range(col_parts)
            ],
            axis=1,
        )
        right = jnp.concatenate(
            [right_ref[:, col ^ q, c].reshape(row_parts * rows, cols) for q in range(col_parts)], axis=1
        )
        summed = lax.dot_general(left, right, NT, preferred_element_type=F32).astype(BF16)
        for at in range(row_groups):
            for q in range(col_parts):
                out_ref[row ^ at, q, c] = summed[at * rows : (at + 1) * rows, q * cols : (q + 1) * cols]


def output_kernel(summed_ref, gating_ref, gain_hbm, bias_hbm, w_hbm, out_ref, scr, gain_scr, bias_scr, w_scr, sems):
    step = pl.program_id(0)
    hidden, rows, cols = summed_ref.shape
    block = out_ref.shape[0]

    @pl.when(step == 0)
    def _():
        waits = start_copies([(gain_hbm, gain_scr), (bias_hbm, bias_scr), (w_hbm, w_scr)], sems)
        values = summed_ref[...].astype(F32)
        average = jnp.sum(values, axis=0, keepdims=True) / hidden
        centred = values - average
        variance = jnp.sum(jnp.square(centred), axis=0, keepdims=True) / hidden
        scr[...] = (centred * lax.rsqrt(variance + EPSILON)).reshape(hidden * rows, cols)
        for wait in waits:
            wait()

    for at in range(block):
        scaled = scr[pl.ds(step * block + at, hidden, stride=rows), :].T
        normed_sum = (scaled * gain_scr[...] + bias_scr[...]).astype(BF16)
        result = jnp.dot(normed_sum, w_scr[...], preferred_element_type=F32)
        out_ref[at] = gating_ref[step * block + at] * result


def exchanged(
    pair_map, pair_mask, in_gain, in_bias, w_proj, w_gate, out_gain, out_bias, w_out, *, row_parts, col_parts
):
    rows, cols, channels = pair_map.shape
    hidden = w_out.shape[0]
    row_groups = row_parts // HALVES
    groups = row_groups * col_parts
    share = hidden // groups
    params = pltpu.CompilerParams(vmem_limit_bytes=VMEM_LIMIT)
    inputs = [in_hbm(x) for x in (pair_map, pair_mask, in_gain.reshape(1, -1), in_bias.reshape(1, -1), w_proj)]
    scratch = [
        pltpu.VMEM((rows, cols, channels), F32),
        pltpu.VMEM((rows, cols), pair_mask.dtype),
        pltpu.VMEM((1, channels), F32),
        pltpu.VMEM((1, channels), F32),
        pltpu.VMEM((channels, 2 * hidden), BF16),
        pltpu.VMEM((2 * hidden, channels), BF16),
        pltpu.VMEM((hidden * rows, cols), F32),
    ]
    right = pl.pallas_call(
        right_kernel,
        in_specs=[HBM] * 5,
        out_specs=VMEM,
        out_shape=jax.ShapeDtypeStruct((HALVES, groups, share, rows, cols), BF16),
        scratch_shapes=scratch + [pltpu.SemaphoreType.DMA((8,))],
        compiler_params=params,
        name="right",
    )(*inputs)
    right = lax.all_to_all(right.reshape(-1, share, rows, cols), ("row", "col"), 0, 0, tiled=True)
    place = {"groups": groups, "row_groups": row_groups, "col_parts": col_parts}
    *lefts, gating = pl.pallas_call(
        functools.partial(left_kernel, **place),
        in_specs=[HBM] * 6,
        out_specs=[VMEM] * (groups + 1),
        out_shape=[jax.ShapeDtypeStruct((share, rows, cols), BF16)] * groups
        + [jax.ShapeDtypeStruct((rows, cols, channels), F32)],
        scratch_shapes=scratch + [pltpu.VMEM(w_gate.shape, BF16), pltpu.SemaphoreType.DMA((9,))],
        compiler_params=params,
        name="left",
    )(*inputs, in_hbm(w_gate))
    devices = range(row_parts * col_parts)
    for offset in range(1, groups):
        lefts[offset] = lax.ppermute(lefts[offset], ("row", "col"), [(n, n ^ offset) for n in devices])
    summed = pl.pallas_call(
        functools.partial(pairs_kernel, row_groups=row_groups, col_parts=col_parts),
        in_specs=[VMEM] * (groups + 1),
        out_specs=VMEM,
        out_shape=jax.ShapeDtypeStruct((row_groups, col_parts, share, rows, cols), BF16),
        compiler_params=params,
        name="pairs",
    )(right.reshape(row_parts, col_parts, share, rows, cols), *lefts)
    halves = [[half * groups + n for n in range(groups)] for half in range(HALVES)]
    summed = lax.all_to_all(
        summed.reshape(groups, share, rows, cols), ("row", "col"), 0, 0, tiled=True, axis_index_groups=halves
    ).reshape(hidden, rows, cols)
    block = rows // 4
    return pl.pallas_call(
        output_kernel,
        grid=(rows // block,),
        in_specs=[VMEM, VMEM, HBM, HBM, HBM],
        out_specs=pl.BlockSpec((block, cols, channels), lambda i: (i, 0, 0)),
        out_shape=jax.ShapeDtypeStruct((rows, cols, channels), F32),
        scratch_shapes=[
            pltpu.VMEM((hidden * rows, cols), F32),
            pltpu.VMEM((1, hidden), F32),
            pltpu.VMEM((1, hidden), F32),
            pltpu.VMEM(w_out.shape, BF16),
            pltpu.SemaphoreType.DMA((3,)),
        ],
        compiler_params=params,
        name="output",
    )(summed, gating, in_hbm(out_gain.reshape(1, -1)), in_hbm(out_bias.reshape(1, -1)), in_hbm(w_out))


def solution(mesh):
    row_parts, col_parts = mesh.shape["row"], mesh.shape["col"]

    def local(pair_map, pair_mask, in_gain, in_bias, w_proj, w_gate, out_gain, out_bias, w_out):
        rows, cols, channels = pair_map.shape
        hidden = w_out.shape[0]
        groups = row_parts // HALVES * col_parts
        whole_tiles = rows % 16 == 0 and cols % 128 == 0 and channels % 128 == 0 and hidden % 128 == 0
        even = row_parts % HALVES == 0 and groups & (groups - 1) == 0 and hidden % groups == 0
        plan = gathered
        if whole_tiles and even:
            plan = functools.partial(exchanged, row_parts=row_parts, col_parts=col_parts)
        return plan(pair_map, pair_mask, in_gain, in_bias, w_proj, w_gate, out_gain, out_bias, w_out)

    in_specs = (P("row", "col", None), P("row", "col"), P(), P(), P(), P(), P(), P(), P())
    out_specs = P("row", "col", None)
    return jax.shard_map(local, mesh=mesh, in_specs=in_specs, out_specs=out_specs, check_vma=False)
```

```python
import functools

import jax
import jax.numpy as jnp
from jax import lax
from jax.experimental import pallas as pl
from jax.experimental.pallas import tpu as pltpu
from jax.sharding import PartitionSpec as P

F32 = jnp.float32
BF16 = jnp.bfloat16
EPSILON = 1e-05
NT = (((1,), (1,)), ((), ()))


def layer_norm(values, gain, bias):
    average = jnp.mean(values, axis=-1, keepdims=True)
    variance = jnp.mean(jnp.square(values - average), axis=-1, keepdims=True)
    return (values - average) * lax.rsqrt(variance + EPSILON) * gain + bias


def gathered(pair_map, pair_mask, in_gain, in_bias, w_proj, w_gate, out_gain, out_bias, w_out):
    row_count, col_count, channels = pair_map.shape
    hidden_width = w_out.shape[0]
    normed_map = layer_norm(pair_map, in_gain, in_bias).astype(BF16)
    flattened = normed_map.reshape(-1, channels)
    projected_all = jnp.dot(flattened, w_proj, preferred_element_type=F32).reshape(
        row_count, col_count, 4 * hidden_width
    )
    masked = pair_mask.astype(F32)[..., None]
    left_side = (
        masked
        * jax.nn.sigmoid(projected_all[..., :hidden_width])
        * projected_all[..., hidden_width : 2 * hidden_width]
    ).astype(BF16)
    gating = jax.nn.sigmoid(jnp.dot(flattened, w_gate, preferred_element_type=F32)).reshape(
        row_count, col_count, channels
    )
    right_side = (
        masked
        * jax.nn.sigmoid(projected_all[..., 2 * hidden_width : 3 * hidden_width])
        * projected_all[..., 3 * hidden_width :]
    ).astype(BF16)
    partial_value = jnp.einsum(
        "ikc,jkc->ijc",
        left_side,
        lax.all_gather(right_side, "row", axis=0, tiled=True),
        preferred_element_type=F32,
    )
    summed = lax.psum_scatter(partial_value, "col", scatter_dimension=1, tiled=True)
    normed_sum = layer_norm(summed, out_gain, out_bias).astype(BF16)
    result = jnp.dot(normed_sum.reshape(-1, hidden_width), w_out, preferred_element_type=F32).reshape(
        row_count, col_count, channels
    )
    return gating * result


HALVES = 2
BLOCKS = 1
CHUNKS = 2
VMEM_LIMIT = 16 * 2**20
HBM = pl.BlockSpec(memory_space=pltpu.MemorySpace.HBM)
VMEM = pl.BlockSpec(memory_space=pltpu.MemorySpace.VMEM)


def gated(gate, value):
    half = 0.5 * value
    return half * jnp.tanh(0.5 * gate) + half


def in_hbm(array):
    return pltpu.with_memory_space_constraint(array, pltpu.MemorySpace.HBM)


def own_place(row_groups, col_parts):
    row, col = lax.axis_index("row"), lax.axis_index("col")
    return lax.rem(row, row_groups), col


def send_order(groups):
    return sorted(range(1, groups), key=lambda offset: -offset.bit_count())


def start_copies(pairs, semaphores):
    copies = [pltpu.make_async_copy(source, target, semaphores.at[n]) for n, (source, target) in enumerate(pairs)]
    for copy in copies:
        copy.start()
    return [copy.wait for copy in copies]


def turned(weights):
    return weights.astype(F32).T.astype(BF16)


def project(normed, w_turned, mask_ref, side_scr, first):
    rows, cols = mask_ref.shape
    hidden = w_turned.shape[0] // 2
    projected = lax.dot_general(w_turned[...], normed, NT, preferred_element_type=F32)
    for at in range(normed.shape[0] // cols):
        row = first + at
        here = projected[:, at * cols : (at + 1) * cols]
        masked = mask_ref[row : row + 1, :].astype(F32)
        side_scr[pl.ds(row, hidden, stride=rows), :] = masked * gated(here[:hidden], here[hidden:])


def right_kernel(map_hbm, mask_hbm, gain_hbm, bias_hbm, w_hbm, out_hbm, normed_ref, map_scr, mask_scr, gain_scr, bias_scr, w_scr, w_turned, side_scr, out_scr, in_sems, out_sems):
    rows, cols, channels = map_scr.shape
    halves, groups, share = out_hbm.shape[:3]
    width = w_scr.shape[1]
    hidden = width // 2
    block = rows // BLOCKS
    *wait_blocks, wait_w, wait_gain, wait_bias, wait_mask = start_copies(
        [(map_hbm.at[pl.ds(n * block, block)], map_scr.at[pl.ds(n * block, block)]) for n in range(BLOCKS)]
        + [
            (w_hbm.at[:, width : 2 * width], w_scr),
            (gain_hbm, gain_scr),
            (bias_hbm, bias_scr),
            (mask_hbm, mask_scr),
        ],
        in_sems,
    )
    wait_w()
    for part in range(2):
        w_turned[part * hidden : (part + 1) * hidden, :] = turned(w_scr[:, part * hidden : (part + 1) * hidden])
    wait_gain()
    wait_bias()
    wait_mask()
    for step, wait_block in enumerate(wait_blocks):
        wait_block()
        values = map_scr[step * block : (step + 1) * block].reshape(block * cols, channels)
        normed = layer_norm(values, gain_scr[...], bias_scr[...]).astype(BF16)
        normed_ref[step * block * cols : (step + 1) * block * cols, :] = normed
        project(normed, w_turned, mask_scr, side_scr, step * block)
    waits = []
    chunk = groups // CHUNKS
    for n in range(CHUNKS):
        span = chunk * share * rows
        side = side_scr[n * span : (n + 1) * span, :].astype(BF16)
        out_scr[n * chunk : (n + 1) * chunk] = side.reshape(chunk, share, rows, cols)
        waits += start_copies(
            [
                (out_scr.at[pl.ds(n * chunk, chunk)], out_hbm.at[half, pl.ds(n * chunk, chunk)])
                for half in range(halves)
            ],
            out_sems.at[pl.ds(n * halves, halves)],
        )
    for wait in waits:
        wait()


def left_kernel(normed_ref, mask_ref, w_ref, *refs, row_groups, col_parts):
    outs, (w_turned, side_scr) = refs[:-2], refs[-2:]
    rows, cols = mask_ref.shape
    share = outs[0].shape[0]
    hidden = w_turned.shape[0] // 2
    for part in range(2):
        w_turned[part * hidden : (part + 1) * hidden, :] = turned(w_ref[:, part * hidden : (part + 1) * hidden])
    block = rows // 4
    for step in range(4):
        normed = normed_ref[step * block * cols : (step + 1) * block * cols, :]
        project(normed, w_turned, mask_ref, side_scr, step * block)
    row, col = own_place(row_groups, col_parts)
    own = row * col_parts + col
    for offset, out_ref in enumerate(outs):
        start = pl.multiple_of((own ^ offset) * (share * rows), share * rows)
        out_ref[...] = side_scr[pl.ds(start, share * rows), :].astype(BF16).reshape(share, rows, cols)


def gates_kernel(normed_ref, w_gate_ref, _, gain_hbm, bias_hbm, w_out_hbm, gating_ref, gain_ref, bias_ref, w_out_ref, sems):
    waits = start_copies([(gain_hbm, gain_ref), (bias_hbm, bias_ref), (w_out_hbm, w_out_ref)], sems)
    rows, cols, channels = gating_ref.shape
    block = rows // 4
    for step in range(4):
        normed = normed_ref[step * block * cols : (step + 1) * block * cols, :]
        gates = jnp.dot(normed, w_gate_ref[...], preferred_element_type=F32)
        gating_ref[step * block : (step + 1) * block] = (0.5 * jnp.tanh(0.5 * gates) + 0.5).reshape(
            block, cols, channels
        )
    for wait in waits:
        wait()


def pairs_kernel(right_ref, *refs, row_groups, col_parts):
    lefts, out_ref = refs[:-2], refs[-1]
    row_parts, _, share, rows, cols = right_ref.shape
    row, col = own_place(row_groups, col_parts)
    for c in range(share):
        left = jnp.concatenate(
            [
                jnp.concatenate([lefts[at * col_parts + q][c] for at in range(row_groups)], axis=0)
                for q in range(col_parts)
            ],
            axis=1,
        )
        right = jnp.concatenate(
            [right_ref[:, col ^ q, c].reshape(row_parts * rows, cols) for q in range(col_parts)], axis=1
        )
        summed = lax.dot_general(left, right, NT, preferred_element_type=F32).astype(BF16)
        for at in range(row_groups):
            for q in range(col_parts):
                out_ref[row ^ at, q, c] = summed[at * rows : (at + 1) * rows, q * cols : (q + 1) * cols]


def output_kernel(summed_ref, gating_ref, gain_ref, bias_ref, w_ref, out_hbm, scr, out_scr, sems):
    hidden, rows, cols = summed_ref.shape
    values = summed_ref[...].astype(F32)
    average = jnp.sum(values, axis=0, keepdims=True) / hidden
    centred = values - average
    variance = jnp.sum(jnp.square(centred), axis=0, keepdims=True) / hidden
    scr[...] = (centred * lax.rsqrt(variance + EPSILON)).reshape(hidden * rows, cols)
    waits = []
    block = rows // sems.shape[0]
    for row in range(rows):
        scaled = scr[pl.ds(row, hidden, stride=rows), :].T
        normed_sum = (scaled * gain_ref[...] + bias_ref[...]).astype(BF16)
        result = jnp.dot(normed_sum, w_ref[...], preferred_element_type=F32)
        out_scr[row] = gating_ref[row] * result
        if (row + 1) % block == 0:
            at = row // block
            ready = pl.ds(at * block, block)
            waits += start_copies([(out_scr.at[ready], out_hbm.at[ready])], sems.at[pl.ds(at, 1)])
    for wait in waits:
        wait()


def exchanged(
    pair_map, pair_mask, in_gain, in_bias, w_proj, w_gate, out_gain, out_bias, w_out, *, row_parts, col_parts
):
    rows, cols, channels = pair_map.shape
    hidden = w_out.shape[0]
    row_groups = row_parts // HALVES
    groups = row_groups * col_parts
    share = hidden // groups
    params = pltpu.CompilerParams(vmem_limit_bytes=VMEM_LIMIT)
    place = {"row_groups": row_groups, "col_parts": col_parts}
    inputs = (pair_map, pair_mask, in_gain.reshape(1, -1), in_bias.reshape(1, -1), w_proj)
    right, normed = pl.pallas_call(
        right_kernel,
        in_specs=[HBM] * 5,
        out_specs=[HBM, VMEM],
        out_shape=[
            pltpu.MemorySpace.HBM((HALVES, groups, share, rows, cols), BF16),
            jax.ShapeDtypeStruct((rows * cols, channels), BF16),
        ],
        scratch_shapes=[
            pltpu.VMEM((rows, cols, channels), F32),
            pltpu.VMEM((rows, cols), pair_mask.dtype),
            pltpu.VMEM((1, channels), F32),
            pltpu.VMEM((1, channels), F32),
            pltpu.VMEM((channels, 2 * hidden), BF16),
            pltpu.VMEM((2 * hidden, channels), BF16),
            pltpu.VMEM((hidden * rows, cols), F32),
            pltpu.VMEM((groups, share, rows, cols), BF16),
            pltpu.SemaphoreType.DMA((BLOCKS + 4,)),
            pltpu.SemaphoreType.DMA((CHUNKS * HALVES,)),
        ],
        compiler_params=params,
        name="right",
    )(*[in_hbm(x) for x in inputs])
    right = lax.all_to_all(right.reshape(-1, share, rows, cols), ("row", "col"), 0, 0, tiled=True)
    lefts = list(pl.pallas_call(
        functools.partial(left_kernel, **place),
        in_specs=[VMEM] * 3,
        out_specs=[VMEM] * groups,
        out_shape=[jax.ShapeDtypeStruct((share, rows, cols), BF16)] * groups,
        scratch_shapes=[pltpu.VMEM((2 * hidden, channels), BF16), pltpu.VMEM((hidden * rows, cols), F32)],
        compiler_params=params,
        name="left",
    )(normed, pair_mask, w_proj))
    devices = range(row_parts * col_parts)
    order = send_order(groups)
    for offset in order:
        lefts[offset] = lax.ppermute(lefts[offset], ("row", "col"), [(n, n ^ offset) for n in devices])
    gating, gain, bias, w_last = pl.pallas_call(
        gates_kernel,
        in_specs=[VMEM, VMEM, VMEM, HBM, HBM, HBM],
        out_specs=[VMEM] * 4,
        out_shape=[
            jax.ShapeDtypeStruct((rows, cols, channels), F32),
            jax.ShapeDtypeStruct((1, hidden), F32),
            jax.ShapeDtypeStruct((1, hidden), F32),
            jax.ShapeDtypeStruct(w_out.shape, BF16),
        ],
        scratch_shapes=[pltpu.SemaphoreType.DMA((3,))],
        compiler_params=params,
        name="gates",
    )(normed, w_gate, lefts[order[0]], in_hbm(out_gain.reshape(1, -1)), in_hbm(out_bias.reshape(1, -1)), in_hbm(w_out))
    summed = pl.pallas_call(
        functools.partial(pairs_kernel, **place),
        in_specs=[VMEM] * (groups + 2),
        out_specs=VMEM,
        out_shape=jax.ShapeDtypeStruct((row_groups, col_parts, share, rows, cols), BF16),
        compiler_params=params,
        name="pairs",
    )(right.reshape(row_parts, col_parts, share, rows, cols), *lefts, gain)
    halves = [[half * groups + n for n in range(groups)] for half in range(HALVES)]
    summed = lax.all_to_all(
        summed.reshape(groups, share, rows, cols), ("row", "col"), 0, 0, tiled=True, axis_index_groups=halves
    ).reshape(hidden, rows, cols)
    return pl.pallas_call(
        output_kernel,
        in_specs=[VMEM] * 5,
        out_specs=HBM,
        out_shape=pltpu.MemorySpace.HBM((rows, cols, channels), F32),
        scratch_shapes=[
            pltpu.VMEM((hidden * rows, cols), F32),
            pltpu.VMEM((rows, cols, channels), F32),
            pltpu.SemaphoreType.DMA((8,)),
        ],
        compiler_params=params,
        name="output",
    )(summed, gating, gain, bias, w_last)


def solution(mesh):
    row_parts, col_parts = mesh.shape["row"], mesh.shape["col"]

    def local(pair_map, pair_mask, in_gain, in_bias, w_proj, w_gate, out_gain, out_bias, w_out):
        rows, cols, channels = pair_map.shape
        hidden = w_out.shape[0]
        groups = row_parts // HALVES * col_parts
        whole_tiles = rows % 16 == 0 and cols % 128 == 0 and channels % 128 == 0 and hidden % 128 == 0
        even = row_parts % HALVES == 0 and groups & (groups - 1) == 0 and hidden % groups == 0
        plan = gathered
        if whole_tiles and even:
            plan = functools.partial(exchanged, row_parts=row_parts, col_parts=col_parts)
        return plan(pair_map, pair_mask, in_gain, in_bias, w_proj, w_gate, out_gain, out_bias, w_out)

    in_specs = (P("row", "col", None), P("row", "col"), P(), P(), P(), P(), P(), P(), P())
    out_specs = P("row", "col", None)
    return jax.shard_map(local, mesh=mesh, in_specs=in_specs, out_specs=out_specs, check_vma=False)
```

```python
import functools

import jax
import jax.numpy as jnp
from jax import lax
from jax.experimental import pallas as pl
from jax.experimental.pallas import tpu as pltpu
from jax.sharding import PartitionSpec as P


F32 = jnp.float32
BF16 = jnp.bfloat16
EPSILON = 1e-05
NT = (((1,), (1,)), ((), ()))


def layer_norm(values, gain, bias):
    average = jnp.mean(values, axis=-1, keepdims=True)
    variance = jnp.mean(jnp.square(values - average), axis=-1, keepdims=True)
    return (values - average) * lax.rsqrt(variance + EPSILON) * gain + bias


def gathered(pair_map, pair_mask, in_gain, in_bias, w_proj, w_gate, out_gain, out_bias, w_out):
    row_count, col_count, channels = pair_map.shape
    hidden_width = w_out.shape[0]
    normed_map = layer_norm(pair_map, in_gain, in_bias).astype(BF16)
    flattened = normed_map.reshape(-1, channels)
    projected_all = jnp.dot(flattened, w_proj, preferred_element_type=F32).reshape(
        row_count, col_count, 4 * hidden_width
    )
    masked = pair_mask.astype(F32)[..., None]
    left_side = (
        masked
        * jax.nn.sigmoid(projected_all[..., :hidden_width])
        * projected_all[..., hidden_width : 2 * hidden_width]
    ).astype(BF16)
    gating = jax.nn.sigmoid(jnp.dot(flattened, w_gate, preferred_element_type=F32)).reshape(
        row_count, col_count, channels
    )
    right_side = (
        masked
        * jax.nn.sigmoid(projected_all[..., 2 * hidden_width : 3 * hidden_width])
        * projected_all[..., 3 * hidden_width :]
    ).astype(BF16)
    partial_value = jnp.einsum(
        "ikc,jkc->ijc",
        left_side,
        lax.all_gather(right_side, "row", axis=0, tiled=True),
        preferred_element_type=F32,
    )
    summed = lax.psum_scatter(partial_value, "col", scatter_dimension=1, tiled=True)
    normed_sum = layer_norm(summed, out_gain, out_bias).astype(BF16)
    result = jnp.dot(normed_sum.reshape(-1, hidden_width), w_out, preferred_element_type=F32).reshape(
        row_count, col_count, channels
    )
    return gating * result


ROW_BITS = 4
GROUPS = 4
VMEM_LIMIT = 16 * 2**20
HBM = pl.BlockSpec(memory_space=pltpu.MemorySpace.HBM)
VMEM = pl.BlockSpec(memory_space=pltpu.MemorySpace.VMEM)


def gated(gate, value):
    half = 0.5 * value
    return half * jnp.tanh(0.5 * gate) + half


def in_hbm(array):
    return pltpu.with_memory_space_constraint(array, pltpu.MemorySpace.HBM)


def own_bits():
    row, col = lax.axis_index("row"), lax.axis_index("col")
    return [(row >> bit) & 1 for bit in reversed(range(ROW_BITS))] + [col]


def start_copies(pairs, semaphores):
    copies = [pltpu.make_async_copy(source, target, semaphores.at[n]) for n, (source, target) in enumerate(pairs)]
    for copy in copies:
        copy.start()
    return [copy.wait for copy in copies]


def turned(weights):
    return weights.astype(F32).T.astype(BF16)


def project(normed, w_turned, mask_ref, side_scr):
    rows, cols = mask_ref.shape
    hidden = side_scr.shape[1] // rows
    for side in range(2):
        weights = w_turned[2 * side * hidden : (2 * side + 2) * hidden, :]
        projected = lax.dot_general(weights, normed, NT, preferred_element_type=F32)
        for row in range(rows):
            here = projected[:, row * cols : (row + 1) * cols]
            masked = mask_ref[row : row + 1, :].astype(F32)
            side_scr[side, pl.ds(row, hidden, stride=rows), :] = masked * gated(here[:hidden], here[hidden:])


def cut(side_scr, side, outs):
    _, _, wide, _, col = own_bits()
    share, rows, cols = outs[0].shape
    for offset, out_ref in enumerate(outs):
        start = pl.multiple_of(((2 * wide + col) ^ offset) * (share * rows), share * rows)
        out_ref[...] = side_scr[side, pl.ds(start, share * rows), :].astype(BF16).reshape(share, rows, cols)


def sides_kernel(map_hbm, mask_hbm, gain_hbm, bias_hbm, w_hbm, *refs):
    lefts, rights, normed_ref = refs[:GROUPS], refs[GROUPS : 2 * GROUPS], refs[2 * GROUPS]
    map_scr, mask_scr, gain_scr, bias_scr, w_scr, w_turned, side_scr, sems = refs[2 * GROUPS + 1 :]
    rows, cols, channels = map_scr.shape
    hidden = w_scr.shape[1] // 4
    wait_map, wait_w, wait_gain, wait_bias, wait_mask = start_copies(
        [(map_hbm, map_scr), (w_hbm, w_scr), (gain_hbm, gain_scr), (bias_hbm, bias_scr), (mask_hbm, mask_scr)], sems
    )
    wait_w()
    for part in range(4):
        w_turned[part * hidden : (part + 1) * hidden, :] = turned(w_scr[:, part * hidden : (part + 1) * hidden])
    wait_gain()
    wait_bias()
    wait_mask()
    wait_map()
    values = map_scr[...].reshape(rows * cols, channels)
    normed = layer_norm(values, gain_scr[...], bias_scr[...]).astype(BF16)
    normed_ref[...] = normed
    project(normed, w_turned, mask_scr, side_scr)
    cut(side_scr, 0, lefts)
    cut(side_scr, 1, rights)


def gates_kernel(normed_ref, w_gate_ref, gain_hbm, bias_hbm, w_out_hbm, gating_ref, gain_ref, bias_ref, w_out_ref, sems):
    waits = start_copies([(gain_hbm, gain_ref), (bias_hbm, bias_ref), (w_out_hbm, w_out_ref)], sems)
    rows, cols, channels = gating_ref.shape
    block = rows // 4
    for step in range(4):
        normed = normed_ref[step * block * cols : (step + 1) * block * cols, :]
        gates = jnp.dot(normed, w_gate_ref[...], preferred_element_type=F32)
        gating_ref[step * block : (step + 1) * block] = (0.5 * jnp.tanh(0.5 * gates) + 0.5).reshape(
            block, cols, channels
        )
    for wait in waits:
        wait()


def pairs_kernel(*refs):
    rights, lefts, out_ref, scr = refs[: 4 * GROUPS], refs[4 * GROUPS : 6 * GROUPS], refs[-2], refs[-1]
    half, parity, wide, core, _ = own_bits()
    share, rows, _ = lefts[0].shape
    for n, piece in enumerate(rights):
        other_core, other_half, other_wide, other_col = [(n >> bit) & 1 for bit in (3, 2, 1, 0)]
        block = 4 * (half ^ other_half) + 2 * (wide ^ other_wide) + (core ^ other_core)
        scr[other_col, :, pl.ds(pl.multiple_of(block * rows, rows), rows), :] = piece[...]
    count = scr.shape[2]
    first = lax.broadcasted_iota(jnp.int32, (GROUPS, rows // 2, count), 2) < count // 2
    for pair in range(share // 2):
        packed = []
        for c in (2 * pair, 2 * pair + 1):
            left = jnp.concatenate(
                [jnp.concatenate([lefts[2 * at + q][c] for at in range(GROUPS)], axis=0) for q in range(2)], axis=1
            )
            right = jnp.concatenate([scr[q, c] for q in range(2)], axis=1)
            summed = lax.dot_general(left, right, NT, preferred_element_type=F32)
            rolled = pltpu.roll(summed, count // 2, 1).reshape(GROUPS, 2, rows // 2, count)
            summed = summed.reshape(GROUPS, 2, rows // 2, count)
            packed.append(
                [
                    jnp.where(first, summed[:, 0], rolled[:, 1]),
                    jnp.where(first, rolled[:, 0], summed[:, 1]),
                ]
            )
        for at in range(GROUPS):
            place = 4 * (parity ^ (at >> 1)) + 2 * (wide ^ (at & 1))
            for q in range(2):
                out_ref[place + q, pair] = jnp.concatenate([packed[0][q][at], packed[1][q][at]], axis=0).astype(BF16)


def output_kernel(summed_ref, gating_ref, gain_ref, bias_ref, w_ref, out_hbm, scr, out_scr, sems):
    rows, cols, _ = out_scr.shape
    hidden = w_ref.shape[0]
    low = rows // 2
    for part in range(2):
        values = summed_ref[part * GROUPS : (part + 1) * GROUPS].astype(F32).reshape(hidden, low, cols)
        average = jnp.sum(values, axis=0, keepdims=True) / hidden
        centred = values - average
        variance = jnp.sum(jnp.square(centred), axis=0, keepdims=True) / hidden
        scr[part] = (centred * lax.rsqrt(variance + EPSILON)).reshape(hidden * low, cols)
    waits = []
    for row in range(low):
        for part in range(2):
            scaled = scr[part, pl.ds(row, hidden, stride=low), :].T
            normed_sum = (scaled * gain_ref[...] + bias_ref[...]).astype(BF16)
            result = jnp.dot(normed_sum, w_ref[...], preferred_element_type=F32)
            for high in range(2):
                at, where = row + high * low, slice(part * cols // 2, (part + 1) * cols // 2)
                out_scr[at, where] = gating_ref[at, where] * result[high * cols // 2 : (high + 1) * cols // 2]
        if row % 2:
            for high in range(2):
                ready = pl.ds(row - 1 + high * low, 2)
                waits += start_copies(
                    [(out_scr.at[ready], out_hbm.at[ready])], sems.at[pl.ds(row // 2 + high * low // 2, 1)]
                )
    for wait in waits:
        wait()


def exchanged(pair_map, pair_mask, in_gain, in_bias, w_proj, w_gate, out_gain, out_bias, w_out, *, col_parts):
    rows, cols, channels = pair_map.shape
    hidden = w_out.shape[0]
    share = hidden // GROUPS
    half, parity, wide, core, col = [col_parts << bit for bit in reversed(range(ROW_BITS))] + [1]
    plane = [0, col, wide, wide + col]
    devices = range(2 * half)

    def swap(array, offset):
        if not offset:
            return array
        return lax.ppermute(array, ("row", "col"), [(n, n ^ offset) for n in devices])

    params = pltpu.CompilerParams(vmem_limit_bytes=VMEM_LIMIT)
    inputs = (pair_map, pair_mask, in_gain.reshape(1, -1), in_bias.reshape(1, -1), w_proj)
    piece = jax.ShapeDtypeStruct((share, rows, cols), BF16)
    *pieces, normed = pl.pallas_call(
        sides_kernel,
        in_specs=[HBM] * 5,
        out_specs=[VMEM] * (2 * GROUPS + 1),
        out_shape=[piece] * (2 * GROUPS) + [jax.ShapeDtypeStruct((rows * cols, channels), BF16)],
        scratch_shapes=[
            pltpu.VMEM((rows, cols, channels), F32),
            pltpu.VMEM((rows, cols), pair_mask.dtype),
            pltpu.VMEM((1, channels), F32),
            pltpu.VMEM((1, channels), F32),
            pltpu.VMEM((channels, 4 * hidden), BF16),
            pltpu.VMEM((4 * hidden, channels), BF16),
            pltpu.VMEM((2, hidden * rows, cols), F32),
            pltpu.SemaphoreType.DMA((5,)),
        ],
        compiler_params=params,
        name="sides",
    )(*[in_hbm(x) for x in inputs])
    lefts, rights = pieces[:GROUPS], pieces[GROUPS:]
    lefts = [swap(x, plane[n]) for n, x in enumerate(lefts)]
    lefts += [swap(x, parity) for x in lefts]
    rights = [swap(x, plane[n]) for n, x in enumerate(rights)]
    rights += [swap(x, half) for x in rights]
    rights += [swap(x, core) for x in rights]
    gating, gain, bias, w_last = pl.pallas_call(
        gates_kernel,
        in_specs=[VMEM, VMEM, HBM, HBM, HBM],
        out_specs=[VMEM] * 4,
        out_shape=[
            jax.ShapeDtypeStruct((rows, cols, channels), F32),
            jax.ShapeDtypeStruct((1, hidden), F32),
            jax.ShapeDtypeStruct((1, hidden), F32),
            jax.ShapeDtypeStruct(w_out.shape, BF16),
        ],
        scratch_shapes=[pltpu.SemaphoreType.DMA((3,))],
        compiler_params=params,
        name="gates",
    )(normed, w_gate, in_hbm(out_gain.reshape(1, -1)), in_hbm(out_bias.reshape(1, -1)), in_hbm(w_out))
    summed = pl.pallas_call(
        pairs_kernel,
        in_specs=[VMEM] * (6 * GROUPS + 1),
        out_specs=VMEM,
        out_shape=jax.ShapeDtypeStruct((2 * GROUPS, share // 2, rows, cols), BF16),
        scratch_shapes=[pltpu.VMEM((2, share, 8 * rows, cols), BF16)],
        compiler_params=params,
        name="pairs",
    )(*rights, *lefts, gain)
    circles = [
        [own + other + offset for other in (0, parity) for offset in plane]
        for own in (0, core, half, half + core)
    ]
    summed = lax.all_to_all(summed, ("row", "col"), 0, 0, tiled=True, axis_index_groups=circles)
    return pl.pallas_call(
        output_kernel,
        in_specs=[VMEM] * 5,
        out_specs=HBM,
        out_shape=pltpu.MemorySpace.HBM((rows, cols, channels), F32),
        scratch_shapes=[
            pltpu.VMEM((2, hidden * rows // 2, cols), F32),
            pltpu.VMEM((rows, cols, channels), F32),
            pltpu.SemaphoreType.DMA((rows // 2,)),
        ],
        compiler_params=params,
        name="output",
    )(summed, gating, gain, bias, w_last)


def solution(mesh):
    row_parts, col_parts = mesh.shape["row"], mesh.shape["col"]

    def local(pair_map, pair_mask, in_gain, in_bias, w_proj, w_gate, out_gain, out_bias, w_out):
        rows, cols, channels = pair_map.shape
        hidden = w_out.shape[0]
        whole_tiles = rows % 16 == 0 and cols % 128 == 0 and channels % 128 == 0 and hidden % 128 == 0
        bits = row_parts == 2**ROW_BITS and col_parts == 2 and rows * row_parts == col_parts * cols
        plan = gathered
        if whole_tiles and bits:
            plan = functools.partial(exchanged, col_parts=col_parts)
        return plan(pair_map, pair_mask, in_gain, in_bias, w_proj, w_gate, out_gain, out_bias, w_out)

    in_specs = (P("row", "col", None), P("row", "col"), P(), P(), P(), P(), P(), P(), P())
    out_specs = P("row", "col", None)
    return jax.shard_map(local, mesh=mesh, in_specs=in_specs, out_specs=out_specs, check_vma=False)
```

```python
import functools

import jax
import jax.numpy as jnp
from jax import lax
from jax.experimental import pallas as pl
from jax.experimental.pallas import tpu as pltpu
from jax.sharding import PartitionSpec as P


F32 = jnp.float32
BF16 = jnp.bfloat16
EPSILON = 1e-05
NT = (((1,), (1,)), ((), ()))


def layer_norm(values, gain, bias):
    average = jnp.mean(values, axis=-1, keepdims=True)
    variance = jnp.mean(jnp.square(values - average), axis=-1, keepdims=True)
    return (values - average) * lax.rsqrt(variance + EPSILON) * gain + bias


def gathered(pair_map, pair_mask, in_gain, in_bias, w_proj, w_gate, out_gain, out_bias, w_out):
    row_count, col_count, channels = pair_map.shape
    hidden_width = w_out.shape[0]
    normed_map = layer_norm(pair_map, in_gain, in_bias).astype(BF16)
    flattened = normed_map.reshape(-1, channels)
    projected_all = jnp.dot(flattened, w_proj, preferred_element_type=F32).reshape(
        row_count, col_count, 4 * hidden_width
    )
    masked = pair_mask.astype(F32)[..., None]
    left_side = (
        masked
        * jax.nn.sigmoid(projected_all[..., :hidden_width])
        * projected_all[..., hidden_width : 2 * hidden_width]
    ).astype(BF16)
    gating = jax.nn.sigmoid(jnp.dot(flattened, w_gate, preferred_element_type=F32)).reshape(
        row_count, col_count, channels
    )
    right_side = (
        masked
        * jax.nn.sigmoid(projected_all[..., 2 * hidden_width : 3 * hidden_width])
        * projected_all[..., 3 * hidden_width :]
    ).astype(BF16)
    partial_value = jnp.einsum(
        "ikc,jkc->ijc",
        left_side,
        lax.all_gather(right_side, "row", axis=0, tiled=True),
        preferred_element_type=F32,
    )
    summed = lax.psum_scatter(partial_value, "col", scatter_dimension=1, tiled=True)
    normed_sum = layer_norm(summed, out_gain, out_bias).astype(BF16)
    result = jnp.dot(normed_sum.reshape(-1, hidden_width), w_out, preferred_element_type=F32).reshape(
        row_count, col_count, channels
    )
    return gating * result


ROW_BITS = 4
GROUPS = 4
VMEM_LIMIT = 16 * 2**20
HBM = pl.BlockSpec(memory_space=pltpu.MemorySpace.HBM)
VMEM = pl.BlockSpec(memory_space=pltpu.MemorySpace.VMEM)


def gated(half_gate, half_value):
    return half_value * jnp.tanh(half_gate) + half_value


def in_hbm(array):
    return pltpu.with_memory_space_constraint(array, pltpu.MemorySpace.HBM)


def own_bits():
    row, col = lax.axis_index("row"), lax.axis_index("col")
    return [(row >> bit) & 1 for bit in reversed(range(ROW_BITS))] + [col]


def start_copies(pairs, semaphores):
    copies = [pltpu.make_async_copy(source, target, semaphores.at[n]) for n, (source, target) in enumerate(pairs)]
    for copy in copies:
        copy.start()
    return [copy.wait for copy in copies]


def turn(w_ref, w_turned):
    hidden = w_ref.shape[1] // 2
    for part, scale in enumerate((0.5, 1.0)):
        columns = w_ref[:, part * hidden : (part + 1) * hidden].astype(F32)
        w_turned[part * hidden : (part + 1) * hidden, :] = (scale * columns).T.astype(BF16)


def project(normed, w_turned, mask_ref, side_scr, first):
    rows, cols = mask_ref.shape
    hidden = w_turned.shape[0] // 2
    projected = lax.dot_general(w_turned[...], normed, NT, preferred_element_type=F32)
    for at in range(normed.shape[0] // cols):
        row = first + at
        here = projected[:, at * cols : (at + 1) * cols]
        half_masked = 0.5 * mask_ref[row : row + 1, :].astype(F32)
        side_scr[pl.ds(row, hidden, stride=rows), :] = gated(here[:hidden], half_masked * here[hidden:])


def cut(side_scr, outs):
    _, _, wide, _, col = own_bits()
    share, rows, cols = outs[0].shape
    for offset, out_ref in enumerate(outs):
        start = pl.multiple_of(((2 * wide + col) ^ offset) * (share * rows), share * rows)
        out_ref[...] = side_scr[pl.ds(start, share * rows), :].astype(BF16).reshape(share, rows, cols)


def right_kernel(map_hbm, mask_hbm, gain_hbm, bias_hbm, w_hbm, *refs):
    outs, normed_ref = refs[:GROUPS], refs[GROUPS]
    map_scr, mask_scr, gain_scr, bias_scr, w_scr, w_turned, side_scr, sems = refs[GROUPS + 1 :]
    rows, cols, channels = map_scr.shape
    width = w_scr.shape[1]
    wait_map, wait_w, wait_gain, wait_bias, wait_mask = start_copies(
        [
            (map_hbm, map_scr),
            (w_hbm.at[:, width : 2 * width], w_scr),
            (gain_hbm, gain_scr),
            (bias_hbm, bias_scr),
            (mask_hbm, mask_scr),
        ],
        sems,
    )
    wait_w()
    turn(w_scr, w_turned)
    wait_gain()
    wait_bias()
    wait_mask()
    wait_map()
    values = map_scr[...].reshape(rows * cols, channels)
    normed = layer_norm(values, gain_scr[...], bias_scr[...]).astype(BF16)
    normed_ref[...] = normed
    project(normed, w_turned, mask_scr, side_scr, 0)
    cut(side_scr, outs)


def left_kernel(normed_ref, mask_ref, w_ref, *refs):
    outs, (w_turned, side_scr) = refs[:GROUPS], refs[GROUPS:]
    rows, cols = mask_ref.shape
    turn(w_ref.at[:, : w_ref.shape[1] // 2], w_turned)
    block = rows // 4
    for step in range(4):
        normed = normed_ref[step * block * cols : (step + 1) * block * cols, :]
        project(normed, w_turned, mask_ref, side_scr, step * block)
    cut(side_scr, outs)


def lay_out(pieces, out_ref):
    _, _, wide, core, _ = own_bits()
    rows = pieces[0].shape[1]
    for n, piece in enumerate(pieces):
        block = 2 * (wide ^ ((n >> 1) & 1)) + (core ^ (n >> 2))
        out_ref[n & 1, :, pl.ds(pl.multiple_of(block * rows, rows), rows), :] = piece[...]


def gates_kernel(normed_ref, w_gate_ref, *refs):
    pieces, (gain_hbm, bias_hbm, w_out_hbm) = refs[: 2 * GROUPS], refs[2 * GROUPS : 2 * GROUPS + 3]
    gating_ref, gain_ref, bias_ref, w_out_ref, near_ref, sems = refs[2 * GROUPS + 3 :]
    waits = start_copies([(gain_hbm, gain_ref), (bias_hbm, bias_ref), (w_out_hbm, w_out_ref)], sems)
    rows, cols, channels = gating_ref.shape
    block = rows // 4
    for step in range(4):
        normed = normed_ref[step * block * cols : (step + 1) * block * cols, :]
        gates = jnp.dot(normed, w_gate_ref[...], preferred_element_type=F32)
        gating_ref[step * block : (step + 1) * block] = (0.5 * jnp.tanh(0.5 * gates) + 0.5).reshape(
            block, cols, channels
        )
    lay_out(pieces, near_ref)
    for wait in waits:
        wait()


def pairs_kernel(near_ref, *refs):
    pieces, lefts, (out_ref, far_scr) = refs[: 2 * GROUPS], refs[2 * GROUPS : 4 * GROUPS], refs[4 * GROUPS :]
    half, parity, wide, _, _ = own_bits()
    share, rows, _ = lefts[0].shape
    lay_out(pieces, far_scr)
    count = 2 * far_scr.shape[2]
    first = lax.broadcasted_iota(jnp.int32, (GROUPS, rows // 2, count), 2) < count // 2
    for pair in range(share // 2):
        packed = []
        for c in (2 * pair, 2 * pair + 1):
            left = jnp.concatenate(
                [jnp.concatenate([lefts[2 * at + q][c] for at in range(GROUPS)], axis=0) for q in range(2)], axis=1
            )
            right = jnp.concatenate(
                [jnp.concatenate([near_ref[q, c], far_scr[q, c]], axis=0) for q in range(2)], axis=1
            )
            summed = lax.dot_general(left, right, NT, preferred_element_type=F32)
            rolled = pltpu.roll(summed, count // 2, 1).reshape(GROUPS, 2, rows // 2, count)
            summed = summed.reshape(GROUPS, 2, rows // 2, count)
            packed.append(
                [
                    jnp.where(first, summed[:, 0], rolled[:, 1]),
                    jnp.where(first, rolled[:, 0], summed[:, 1]),
                ]
            )
        for at in range(GROUPS):
            place = 4 * (parity ^ (at >> 1)) + 2 * (wide ^ (at & 1))
            for q in range(2):
                sums = jnp.concatenate([packed[0][q][at], packed[1][q][at]], axis=0)
                out_ref[place + (half ^ q), pair] = sums.astype(BF16)


def output_kernel(summed_ref, gating_ref, gain_ref, bias_ref, w_ref, out_hbm, scr, out_scr, sems):
    rows, cols, _ = out_scr.shape
    hidden = w_ref.shape[0]
    low = rows // 2
    for part in range(2):
        values = summed_ref[part * GROUPS : (part + 1) * GROUPS].astype(F32).reshape(hidden, low, cols)
        average = jnp.sum(values, axis=0, keepdims=True) / hidden
        centred = values - average
        variance = jnp.sum(jnp.square(centred), axis=0, keepdims=True) / hidden
        scr[part] = (centred * lax.rsqrt(variance + EPSILON)).reshape(hidden * low, cols)
    waits = []
    for row in range(low):
        for part in range(2):
            scaled = scr[part, pl.ds(row, hidden, stride=low), :].T
            normed_sum = (scaled * gain_ref[...] + bias_ref[...]).astype(BF16)
            result = jnp.dot(normed_sum, w_ref[...], preferred_element_type=F32)
            for high in range(2):
                at, where = row + high * low, slice(part * cols // 2, (part + 1) * cols // 2)
                out_scr[at, where] = gating_ref[at, where] * result[high * cols // 2 : (high + 1) * cols // 2]
        if row % 2:
            for high in range(2):
                ready = pl.ds(row - 1 + high * low, 2)
                waits += start_copies(
                    [(out_scr.at[ready], out_hbm.at[ready])], sems.at[pl.ds(row // 2 + high * low // 2, 1)]
                )
    for wait in waits:
        wait()


def exchanged(pair_map, pair_mask, in_gain, in_bias, w_proj, w_gate, out_gain, out_bias, w_out, *, col_parts):
    rows, cols, channels = pair_map.shape
    hidden = w_out.shape[0]
    share = hidden // GROUPS
    half, parity, wide, core, col = [col_parts << bit for bit in reversed(range(ROW_BITS))] + [1]
    plane = [0, col, wide, wide + col]
    devices = range(2 * half)

    def swap(array, offset):
        if not offset:
            return array
        return lax.ppermute(array, ("row", "col"), [(n, n ^ offset) for n in devices])

    params = pltpu.CompilerParams(vmem_limit_bytes=VMEM_LIMIT)
    inputs = (pair_map, pair_mask, in_gain.reshape(1, -1), in_bias.reshape(1, -1), w_proj)
    piece = jax.ShapeDtypeStruct((share, rows, cols), BF16)
    laid_out = jax.ShapeDtypeStruct((2, share, 4 * rows, cols), BF16)
    turned_shape = pltpu.VMEM((2 * hidden, channels), BF16)
    side_shape = pltpu.VMEM((hidden * rows, cols), F32)
    *rights, normed = pl.pallas_call(
        right_kernel,
        in_specs=[HBM] * 5,
        out_specs=[VMEM] * (GROUPS + 1),
        out_shape=[piece] * GROUPS + [jax.ShapeDtypeStruct((rows * cols, channels), BF16)],
        scratch_shapes=[
            pltpu.VMEM((rows, cols, channels), F32),
            pltpu.VMEM((rows, cols), pair_mask.dtype),
            pltpu.VMEM((1, channels), F32),
            pltpu.VMEM((1, channels), F32),
            pltpu.VMEM((channels, 2 * hidden), BF16),
            turned_shape,
            side_shape,
            pltpu.SemaphoreType.DMA((5,)),
        ],
        compiler_params=params,
        name="right",
    )(*[in_hbm(x) for x in inputs])
    lefts = pl.pallas_call(
        left_kernel,
        in_specs=[VMEM] * 3,
        out_specs=[VMEM] * GROUPS,
        out_shape=[piece] * GROUPS,
        scratch_shapes=[turned_shape, side_shape],
        compiler_params=params,
        name="left",
    )(normed, pair_mask, w_proj)
    lefts = [swap(x, plane[n]) for n, x in enumerate(lefts)]
    lefts += [swap(x, parity) for x in lefts]
    rights = [swap(x, plane[n]) for n, x in enumerate(rights)]
    rights += [swap(x, half) for x in rights]
    across = [swap(x, core) for x in rights]
    gating, gain, bias, w_last, near = pl.pallas_call(
        gates_kernel,
        in_specs=[VMEM] * (2 * GROUPS + 2) + [HBM] * 3,
        out_specs=[VMEM] * 5,
        out_shape=[
            jax.ShapeDtypeStruct((rows, cols, channels), F32),
            jax.ShapeDtypeStruct((1, hidden), F32),
            jax.ShapeDtypeStruct((1, hidden), F32),
            jax.ShapeDtypeStruct(w_out.shape, BF16),
            laid_out,
        ],
        scratch_shapes=[pltpu.SemaphoreType.DMA((3,))],
        compiler_params=params,
        name="gates",
    )(
        normed,
        w_gate,
        *rights[:GROUPS],
        *across[:GROUPS],
        in_hbm(out_gain.reshape(1, -1)),
        in_hbm(out_bias.reshape(1, -1)),
        in_hbm(w_out),
    )
    summed = pl.pallas_call(
        pairs_kernel,
        in_specs=[VMEM] * (4 * GROUPS + 1),
        out_specs=VMEM,
        out_shape=jax.ShapeDtypeStruct((2 * GROUPS, share // 2, rows, cols), BF16),
        scratch_shapes=[pltpu.VMEM(laid_out.shape, BF16)],
        compiler_params=params,
        name="pairs",
    )(near, *rights[GROUPS:], *across[GROUPS:], *lefts)
    circles = [
        [own + other + offset for other in (0, parity) for offset in plane]
        for own in (0, core, half, half + core)
    ]
    summed = lax.all_to_all(summed, ("row", "col"), 0, 0, tiled=True, axis_index_groups=circles)
    return pl.pallas_call(
        output_kernel,
        in_specs=[VMEM] * 5,
        out_specs=HBM,
        out_shape=pltpu.MemorySpace.HBM((rows, cols, channels), F32),
        scratch_shapes=[
            pltpu.VMEM((2, hidden * rows // 2, cols), F32),
            pltpu.VMEM((rows, cols, channels), F32),
            pltpu.SemaphoreType.DMA((rows // 2,)),
        ],
        compiler_params=params,
        name="output",
    )(summed, gating, gain, bias, w_last)


def solution(mesh):
    row_parts, col_parts = mesh.shape["row"], mesh.shape["col"]

    def local(pair_map, pair_mask, in_gain, in_bias, w_proj, w_gate, out_gain, out_bias, w_out):
        rows, cols, channels = pair_map.shape
        hidden = w_out.shape[0]
        whole_tiles = rows % 16 == 0 and cols % 128 == 0 and channels % 128 == 0 and hidden % 128 == 0
        bits = row_parts == 2**ROW_BITS and col_parts == 2 and rows * row_parts == col_parts * cols
        plan = gathered
        if whole_tiles and bits:
            plan = functools.partial(exchanged, col_parts=col_parts)
        return plan(pair_map, pair_mask, in_gain, in_bias, w_proj, w_gate, out_gain, out_bias, w_out)

    in_specs = (P("row", "col", None), P("row", "col"), P(), P(), P(), P(), P(), P(), P())
    out_specs = P("row", "col", None)
    return jax.shard_map(local, mesh=mesh, in_specs=in_specs, out_specs=out_specs, check_vma=False)
```

```python
import functools

import jax
import jax.numpy as jnp
from jax import lax
from jax.experimental import pallas as pl
from jax.experimental.pallas import tpu as pltpu
from jax.sharding import PartitionSpec as P


F32 = jnp.float32
BF16 = jnp.bfloat16
EPSILON = 1e-05
NT = (((1,), (1,)), ((), ()))


def layer_norm(values, gain, bias):
    average = jnp.mean(values, axis=-1, keepdims=True)
    variance = jnp.mean(jnp.square(values - average), axis=-1, keepdims=True)
    return (values - average) * lax.rsqrt(variance + EPSILON) * gain + bias


def gathered(pair_map, pair_mask, in_gain, in_bias, w_proj, w_gate, out_gain, out_bias, w_out):
    row_count, col_count, channels = pair_map.shape
    hidden_width = w_out.shape[0]
    normed_map = layer_norm(pair_map, in_gain, in_bias).astype(BF16)
    flattened = normed_map.reshape(-1, channels)
    projected_all = jnp.dot(flattened, w_proj, preferred_element_type=F32).reshape(
        row_count, col_count, 4 * hidden_width
    )
    masked = pair_mask.astype(F32)[..., None]
    left_side = (
        masked
        * jax.nn.sigmoid(projected_all[..., :hidden_width])
        * projected_all[..., hidden_width : 2 * hidden_width]
    ).astype(BF16)
    gating = jax.nn.sigmoid(jnp.dot(flattened, w_gate, preferred_element_type=F32)).reshape(
        row_count, col_count, channels
    )
    right_side = (
        masked
        * jax.nn.sigmoid(projected_all[..., 2 * hidden_width : 3 * hidden_width])
        * projected_all[..., 3 * hidden_width :]
    ).astype(BF16)
    partial_value = jnp.einsum(
        "ikc,jkc->ijc",
        left_side,
        lax.all_gather(right_side, "row", axis=0, tiled=True),
        preferred_element_type=F32,
    )
    summed = lax.psum_scatter(partial_value, "col", scatter_dimension=1, tiled=True)
    normed_sum = layer_norm(summed, out_gain, out_bias).astype(BF16)
    result = jnp.dot(normed_sum.reshape(-1, hidden_width), w_out, preferred_element_type=F32).reshape(
        row_count, col_count, channels
    )
    return gating * result


ROW_BITS = 4
GROUPS = 4
BLOCKS = 4
VMEM_LIMIT = 16 * 2**20
HBM = pl.BlockSpec(memory_space=pltpu.MemorySpace.HBM)
VMEM = pl.BlockSpec(memory_space=pltpu.MemorySpace.VMEM)


def gated(half_gate, half_value):
    return half_value * jnp.tanh(half_gate) + half_value


def in_hbm(array):
    return pltpu.with_memory_space_constraint(array, pltpu.MemorySpace.HBM)


def own_bits():
    row, col = lax.axis_index("row"), lax.axis_index("col")
    return [(row >> bit) & 1 for bit in reversed(range(ROW_BITS))] + [col]


def start_copies(pairs, semaphores):
    copies = [pltpu.make_async_copy(source, target, semaphores.at[n]) for n, (source, target) in enumerate(pairs)]
    for copy in copies:
        copy.start()
    return [copy.wait for copy in copies]


def turn(w_ref, first, w_turned):
    hidden = w_turned.shape[0] // 2
    for part, scale in enumerate((0.5, 1.0)):
        columns = w_ref[:, first + part * hidden : first + (part + 1) * hidden].astype(F32)
        w_turned[part * hidden : (part + 1) * hidden, :] = (scale * columns).T.astype(BF16)


def project(normed, w_turned, first, mask_ref, side_scr, row):
    rows, cols = mask_ref.shape
    hidden, count = w_turned.shape[0] // 2, side_scr.shape[0] // rows
    weights = [w_turned[pl.ds(pl.multiple_of(start + first, count), count), :] for start in (0, hidden)]
    projected = lax.dot_general(jnp.concatenate(weights, axis=0), normed, NT, preferred_element_type=F32)
    for at in range(normed.shape[0] // cols):
        here = projected[:, at * cols : (at + 1) * cols]
        half_masked = 0.5 * mask_ref[row + at : row + at + 1, :].astype(F32)
        side_scr[pl.ds(row + at, count, stride=rows), :] = gated(here[:count], half_masked * here[count:])


def cut(side_scr, own, outs):
    share, rows, cols = outs[0].shape
    for offset, out_ref in enumerate(outs):
        start = pl.multiple_of((own ^ offset) * (share * rows), share * rows)
        out_ref[...] = side_scr[pl.ds(start, share * rows), :].astype(BF16).reshape(share, rows, cols)


def right_kernel(map_hbm, mask_hbm, gain_hbm, bias_hbm, w_hbm, *refs):
    outs, normed_ref = refs[: GROUPS // 2], refs[GROUPS // 2]
    map_scr, mask_scr, gain_scr, bias_scr, w_scr, w_turned, side_scr, sems = refs[GROUPS // 2 + 1 :]
    rows, cols, channels = map_scr.shape
    width = w_scr.shape[1]
    _, _, wide, _, col = own_bits()
    wait_map, wait_w, wait_gain, wait_bias, wait_mask = start_copies(
        [
            (map_hbm, map_scr),
            (w_hbm.at[:, width : 2 * width], w_scr),
            (gain_hbm, gain_scr),
            (bias_hbm, bias_scr),
            (mask_hbm, mask_scr),
        ],
        sems,
    )
    wait_w()
    turn(w_scr, 0, w_turned)
    wait_gain()
    wait_bias()
    wait_mask()
    wait_map()
    block = rows // BLOCKS
    for row in range(0, rows, block):
        values = map_scr[row : row + block].reshape(block * cols, channels)
        normed = layer_norm(values, gain_scr[...], bias_scr[...]).astype(BF16)
        normed_ref[row * cols : (row + block) * cols, :] = normed
        project(normed, w_turned, wide * (width // 4), mask_scr, side_scr, row)
    cut(side_scr, col, outs)


def left_kernel(normed_ref, mask_ref, w_ref, *refs):
    rights, lefts = refs[: GROUPS // 2], refs[GROUPS // 2 : GROUPS // 2 + GROUPS]
    w_turned, right_scr, left_scr = refs[GROUPS // 2 + GROUPS :]
    rows, cols = mask_ref.shape
    width = w_ref.shape[1] // 2
    _, _, wide, _, col = own_bits()
    block = rows // BLOCKS
    sides = ((0, left_scr, 0, 2 * wide + col, lefts), (width, right_scr, (wide ^ 1) * (width // 4), col, rights))
    for start, side_scr, first, own, outs in sides:
        turn(w_ref, start, w_turned)
        for row in range(0, rows, block):
            normed = normed_ref[row * cols : (row + block) * cols, :]
            project(normed, w_turned, first, mask_ref, side_scr, row)
        cut(side_scr, own, outs)


def lay_out(pieces, out_ref):
    _, _, wide, core, _ = own_bits()
    rows = pieces[0].shape[1]
    for n, piece in enumerate(pieces):
        block = 2 * (wide ^ ((n >> 1) & 1)) + (core ^ (n >> 2))
        out_ref[n & 1, :, pl.ds(pl.multiple_of(block * rows, rows), rows), :] = piece[...]


def gates_kernel(normed_ref, w_gate_ref, *refs):
    pieces, (gain_hbm, bias_hbm, w_out_hbm) = refs[: 2 * GROUPS], refs[2 * GROUPS : 2 * GROUPS + 3]
    gating_ref, gain_ref, bias_ref, w_out_ref, near_ref, sems = refs[2 * GROUPS + 3 :]
    waits = start_copies([(gain_hbm, gain_ref), (bias_hbm, bias_ref), (w_out_hbm, w_out_ref)], sems)
    rows, cols, channels = gating_ref.shape
    block = rows // 4
    for step in range(4):
        normed = normed_ref[step * block * cols : (step + 1) * block * cols, :]
        gates = jnp.dot(normed, w_gate_ref[...], preferred_element_type=F32)
        gating_ref[step * block : (step + 1) * block] = (0.5 * jnp.tanh(0.5 * gates) + 0.5).reshape(
            block, cols, channels
        )
    lay_out(pieces, near_ref)
    for wait in waits:
        wait()


def pairs_kernel(near_ref, *refs):
    pieces, lefts, (out_ref, far_scr) = refs[: 2 * GROUPS], refs[2 * GROUPS : 4 * GROUPS], refs[4 * GROUPS :]
    half, parity, wide, _, _ = own_bits()
    share, rows, _ = lefts[0].shape
    lay_out(pieces, far_scr)
    count = 2 * far_scr.shape[2]
    first = lax.broadcasted_iota(jnp.int32, (GROUPS, rows // 2, count), 2) < count // 2
    for pair in range(share // 2):
        packed = []
        for c in (2 * pair, 2 * pair + 1):
            left = jnp.concatenate(
                [jnp.concatenate([lefts[2 * at + q][c] for at in range(GROUPS)], axis=0) for q in range(2)], axis=1
            )
            right = jnp.concatenate(
                [jnp.concatenate([near_ref[q, c], far_scr[q, c]], axis=0) for q in range(2)], axis=1
            )
            summed = lax.dot_general(left, right, NT, preferred_element_type=F32)
            rolled = pltpu.roll(summed, count // 2, 1).reshape(GROUPS, 2, rows // 2, count)
            summed = summed.reshape(GROUPS, 2, rows // 2, count)
            packed.append(
                [
                    jnp.where(first, summed[:, 0], rolled[:, 1]),
                    jnp.where(first, rolled[:, 0], summed[:, 1]),
                ]
            )
        for at in range(GROUPS):
            place = 4 * (parity ^ (at >> 1)) + 2 * (wide ^ (at & 1))
            for q in range(2):
                sums = jnp.concatenate([packed[0][q][at], packed[1][q][at]], axis=0)
                out_ref[place + (half ^ q), pair] = sums.astype(BF16)


def output_kernel(summed_ref, gating_ref, gain_ref, bias_ref, w_ref, out_hbm, scr, out_scr, sems):
    rows, cols, _ = out_scr.shape
    hidden = w_ref.shape[0]
    low = rows // 2
    for part in range(2):
        values = summed_ref[part * GROUPS : (part + 1) * GROUPS].astype(F32).reshape(hidden, low, cols)
        average = jnp.sum(values, axis=0, keepdims=True) / hidden
        centred = values - average
        variance = jnp.sum(jnp.square(centred), axis=0, keepdims=True) / hidden
        scr[part] = (centred * lax.rsqrt(variance + EPSILON)).reshape(hidden * low, cols)
    waits = []
    for row in range(low):
        for part in range(2):
            scaled = scr[part, pl.ds(row, hidden, stride=low), :].T
            normed_sum = (scaled * gain_ref[...] + bias_ref[...]).astype(BF16)
            result = jnp.dot(normed_sum, w_ref[...], preferred_element_type=F32)
            for high in range(2):
                at, where = row + high * low, slice(part * cols // 2, (part + 1) * cols // 2)
                out_scr[at, where] = gating_ref[at, where] * result[high * cols // 2 : (high + 1) * cols // 2]
        if row % 2:
            for high in range(2):
                ready = pl.ds(row - 1 + high * low, 2)
                waits += start_copies(
                    [(out_scr.at[ready], out_hbm.at[ready])], sems.at[pl.ds(row // 2 + high * low // 2, 1)]
                )
    for wait in waits:
        wait()


def exchanged(pair_map, pair_mask, in_gain, in_bias, w_proj, w_gate, out_gain, out_bias, w_out, *, col_parts):
    rows, cols, channels = pair_map.shape
    hidden = w_out.shape[0]
    share = hidden // GROUPS
    half, parity, wide, core, col = [col_parts << bit for bit in reversed(range(ROW_BITS))] + [1]
    plane = [0, col, wide, wide + col]
    devices = range(2 * half)

    def swap(array, offset):
        if not offset:
            return array
        return lax.ppermute(array, ("row", "col"), [(n, n ^ offset) for n in devices])

    params = pltpu.CompilerParams(vmem_limit_bytes=VMEM_LIMIT)
    inputs = (pair_map, pair_mask, in_gain.reshape(1, -1), in_bias.reshape(1, -1), w_proj)
    piece = jax.ShapeDtypeStruct((share, rows, cols), BF16)
    laid_out = jax.ShapeDtypeStruct((2, share, 4 * rows, cols), BF16)
    turned_shape = pltpu.VMEM((2 * hidden, channels), BF16)
    *rights, normed = pl.pallas_call(
        right_kernel,
        in_specs=[HBM] * 5,
        out_specs=[VMEM] * (GROUPS // 2 + 1),
        out_shape=[piece] * (GROUPS // 2) + [jax.ShapeDtypeStruct((rows * cols, channels), BF16)],
        scratch_shapes=[
            pltpu.VMEM((rows, cols, channels), F32),
            pltpu.VMEM((rows, cols), pair_mask.dtype),
            pltpu.VMEM((1, channels), F32),
            pltpu.VMEM((1, channels), F32),
            pltpu.VMEM((channels, 2 * hidden), BF16),
            turned_shape,
            pltpu.VMEM((hidden // 2 * rows, cols), F32),
            pltpu.SemaphoreType.DMA((5,)),
        ],
        compiler_params=params,
        name="right",
    )(*[in_hbm(x) for x in inputs])
    pieces = pl.pallas_call(
        left_kernel,
        in_specs=[VMEM] * 3,
        out_specs=[VMEM] * (GROUPS // 2 + GROUPS),
        out_shape=[piece] * (GROUPS // 2 + GROUPS),
        scratch_shapes=[
            turned_shape,
            pltpu.VMEM((hidden // 2 * rows, cols), F32),
            pltpu.VMEM((hidden * rows, cols), F32),
        ],
        compiler_params=params,
        name="left",
    )(normed, pair_mask, w_proj)
    rights, lefts = [*rights, *pieces[: GROUPS // 2]], pieces[GROUPS // 2 :]
    lefts = [swap(x, plane[n]) for n, x in enumerate(lefts)]
    lefts += [swap(x, parity) for x in lefts]
    rights = [swap(x, plane[n]) for n, x in enumerate(rights)]
    rights += [swap(x, half) for x in rights]
    across = [swap(x, core) for x in rights]
    gating, gain, bias, w_last, near = pl.pallas_call(
        gates_kernel,
        in_specs=[VMEM] * (2 * GROUPS + 2) + [HBM] * 3,
        out_specs=[VMEM] * 5,
        out_shape=[
            jax.ShapeDtypeStruct((rows, cols, channels), F32),
            jax.ShapeDtypeStruct((1, hidden), F32),
            jax.ShapeDtypeStruct((1, hidden), F32),
            jax.ShapeDtypeStruct(w_out.shape, BF16),
            laid_out,
        ],
        scratch_shapes=[pltpu.SemaphoreType.DMA((3,))],
        compiler_params=params,
        name="gates",
    )(
        normed,
        w_gate,
        *rights[:GROUPS],
        *across[:GROUPS],
        in_hbm(out_gain.reshape(1, -1)),
        in_hbm(out_bias.reshape(1, -1)),
        in_hbm(w_out),
    )
    summed = pl.pallas_call(
        pairs_kernel,
        in_specs=[VMEM] * (4 * GROUPS + 1),
        out_specs=VMEM,
        out_shape=jax.ShapeDtypeStruct((2 * GROUPS, share // 2, rows, cols), BF16),
        scratch_shapes=[pltpu.VMEM(laid_out.shape, BF16)],
        compiler_params=params,
        name="pairs",
    )(near, *rights[GROUPS:], *across[GROUPS:], *lefts)
    circles = [
        [own + other + offset for other in (0, parity) for offset in plane]
        for own in (0, core, half, half + core)
    ]
    summed = lax.all_to_all(summed, ("row", "col"), 0, 0, tiled=True, axis_index_groups=circles)
    return pl.pallas_call(
        output_kernel,
        in_specs=[VMEM] * 5,
        out_specs=HBM,
        out_shape=pltpu.MemorySpace.HBM((rows, cols, channels), F32),
        scratch_shapes=[
            pltpu.VMEM((2, hidden * rows // 2, cols), F32),
            pltpu.VMEM((rows, cols, channels), F32),
            pltpu.SemaphoreType.DMA((rows // 2,)),
        ],
        compiler_params=params,
        name="output",
    )(summed, gating, gain, bias, w_last)


def solution(mesh):
    row_parts, col_parts = mesh.shape["row"], mesh.shape["col"]

    def local(pair_map, pair_mask, in_gain, in_bias, w_proj, w_gate, out_gain, out_bias, w_out):
        rows, cols, channels = pair_map.shape
        hidden = w_out.shape[0]
        whole_tiles = rows % 16 == 0 and cols % 128 == 0 and channels % 128 == 0 and hidden % 128 == 0
        bits = row_parts == 2**ROW_BITS and col_parts == 2 and rows * row_parts == col_parts * cols
        plan = gathered
        if whole_tiles and bits:
            plan = functools.partial(exchanged, col_parts=col_parts)
        return plan(pair_map, pair_mask, in_gain, in_bias, w_proj, w_gate, out_gain, out_bias, w_out)

    in_specs = (P("row", "col", None), P("row", "col"), P(), P(), P(), P(), P(), P(), P())
    out_specs = P("row", "col", None)
    return jax.shard_map(local, mesh=mesh, in_specs=in_specs, out_specs=out_specs, check_vma=False)
```

```python
import functools

import jax
import jax.numpy as jnp
from jax import lax
from jax.experimental import pallas as pl
from jax.experimental.pallas import tpu as pltpu
from jax.sharding import PartitionSpec as P


F32 = jnp.float32
BF16 = jnp.bfloat16
EPSILON = 1e-05
NT = (((1,), (1,)), ((), ()))


def layer_norm(values, gain, bias):
    average = jnp.mean(values, axis=-1, keepdims=True)
    variance = jnp.mean(jnp.square(values - average), axis=-1, keepdims=True)
    return (values - average) * lax.rsqrt(variance + EPSILON) * gain + bias


def gathered(pair_map, pair_mask, in_gain, in_bias, w_proj, w_gate, out_gain, out_bias, w_out):
    row_count, col_count, channels = pair_map.shape
    hidden_width = w_out.shape[0]
    normed_map = layer_norm(pair_map, in_gain, in_bias).astype(BF16)
    flattened = normed_map.reshape(-1, channels)
    projected_all = jnp.dot(flattened, w_proj, preferred_element_type=F32).reshape(
        row_count, col_count, 4 * hidden_width
    )
    masked = pair_mask.astype(F32)[..., None]
    left_side = (
        masked
        * jax.nn.sigmoid(projected_all[..., :hidden_width])
        * projected_all[..., hidden_width : 2 * hidden_width]
    ).astype(BF16)
    gating = jax.nn.sigmoid(jnp.dot(flattened, w_gate, preferred_element_type=F32)).reshape(
        row_count, col_count, channels
    )
    right_side = (
        masked
        * jax.nn.sigmoid(projected_all[..., 2 * hidden_width : 3 * hidden_width])
        * projected_all[..., 3 * hidden_width :]
    ).astype(BF16)
    partial_value = jnp.einsum(
        "ikc,jkc->ijc",
        left_side,
        lax.all_gather(right_side, "row", axis=0, tiled=True),
        preferred_element_type=F32,
    )
    summed = lax.psum_scatter(partial_value, "col", scatter_dimension=1, tiled=True)
    normed_sum = layer_norm(summed, out_gain, out_bias).astype(BF16)
    result = jnp.dot(normed_sum.reshape(-1, hidden_width), w_out, preferred_element_type=F32).reshape(
        row_count, col_count, channels
    )
    return gating * result


ROW_BITS = 4
GROUPS = 4
VMEM_LIMIT = 16 * 2**20
HBM = pl.BlockSpec(memory_space=pltpu.MemorySpace.HBM)
VMEM = pl.BlockSpec(memory_space=pltpu.MemorySpace.VMEM)


def gated(half_gate, half_value):
    return half_value * jnp.tanh(half_gate) + half_value


def in_hbm(array):
    return pltpu.with_memory_space_constraint(array, pltpu.MemorySpace.HBM)


def own_bits():
    row, col = lax.axis_index("row"), lax.axis_index("col")
    return [(row >> bit) & 1 for bit in reversed(range(ROW_BITS))] + [col]


def start_copies(pairs, semaphores):
    copies = [pltpu.make_async_copy(source, target, semaphores.at[n]) for n, (source, target) in enumerate(pairs)]
    for copy in copies:
        copy.start()
    return [copy.wait for copy in copies]


def turn(w_ref, w_turned):
    hidden = w_ref.shape[1] // 2
    for part, scale in enumerate((0.5, 1.0)):
        columns = w_ref[:, part * hidden : (part + 1) * hidden].astype(F32)
        w_turned[part * hidden : (part + 1) * hidden, :] = (scale * columns).T.astype(BF16)


def project(normed, w_turned, mask_ref, side_scr, first):
    rows, cols = mask_ref.shape
    hidden = w_turned.shape[0] // 2
    projected = lax.dot_general(w_turned[...], normed, NT, preferred_element_type=F32)
    for at in range(normed.shape[0] // cols):
        row = first + at
        here = projected[:, at * cols : (at + 1) * cols]
        half_masked = 0.5 * mask_ref[row : row + 1, :].astype(F32)
        side_scr[pl.ds(row, hidden, stride=rows), :] = gated(here[:hidden], half_masked * here[hidden:])


def cut(side_scr, outs):
    _, _, wide, _, col = own_bits()
    share, rows, cols = outs[0].shape
    for offset, out_ref in enumerate(outs):
        start = pl.multiple_of(((2 * wide + col) ^ offset) * (share * rows), share * rows)
        out_ref[...] = side_scr[pl.ds(start, share * rows), :].astype(BF16).reshape(share, rows, cols)


def right_kernel(map_hbm, mask_hbm, gain_hbm, bias_hbm, w_hbm, *refs):
    outs, normed_ref = refs[:GROUPS], refs[GROUPS]
    map_scr, mask_scr, gain_scr, bias_scr, w_scr, w_turned, side_scr, sems = refs[GROUPS + 1 :]
    rows, cols, channels = map_scr.shape
    width = w_scr.shape[1]
    wait_map, wait_w, wait_gain, wait_bias, wait_mask = start_copies(
        [
            (map_hbm, map_scr),
            (w_hbm.at[:, width : 2 * width], w_scr),
            (gain_hbm, gain_scr),
            (bias_hbm, bias_scr),
            (mask_hbm, mask_scr),
        ],
        sems,
    )
    wait_w()
    turn(w_scr, w_turned)
    wait_gain()
    wait_bias()
    wait_mask()
    wait_map()
    block = rows // 4
    for step in range(4):
        values = map_scr[step * block : (step + 1) * block].reshape(block * cols, channels)
        normed = layer_norm(values, gain_scr[...], bias_scr[...]).astype(BF16)
        normed_ref[step * block * cols : (step + 1) * block * cols, :] = normed
        project(normed, w_turned, mask_scr, side_scr, step * block)
    cut(side_scr, outs)


def left_kernel(normed_ref, mask_ref, w_ref, *refs):
    outs, (w_turned, side_scr) = refs[:GROUPS], refs[GROUPS:]
    rows, cols = mask_ref.shape
    turn(w_ref.at[:, : w_ref.shape[1] // 2], w_turned)
    block = rows // 4
    for step in range(4):
        normed = normed_ref[step * block * cols : (step + 1) * block * cols, :]
        project(normed, w_turned, mask_ref, side_scr, step * block)
    cut(side_scr, outs)


def lay_out(pieces, out_ref):
    _, _, wide, core, _ = own_bits()
    rows = pieces[0].shape[1]
    for n, piece in enumerate(pieces):
        block = 2 * (wide ^ ((n >> 1) & 1)) + (core ^ (n >> 2))
        out_ref[n & 1, :, pl.ds(pl.multiple_of(block * rows, rows), rows), :] = piece[...]


def gates_kernel(normed_ref, w_gate_ref, *refs):
    pieces, (gain_hbm, bias_hbm, w_out_hbm) = refs[: 2 * GROUPS], refs[2 * GROUPS : 2 * GROUPS + 3]
    gating_ref, gain_ref, bias_ref, w_out_ref, near_ref, sems = refs[2 * GROUPS + 3 :]
    waits = start_copies([(gain_hbm, gain_ref), (bias_hbm, bias_ref), (w_out_hbm, w_out_ref)], sems)
    rows, cols, channels = gating_ref.shape
    block = rows // 4
    for step in range(4):
        normed = normed_ref[step * block * cols : (step + 1) * block * cols, :]
        gates = jnp.dot(normed, w_gate_ref[...], preferred_element_type=F32)
        gating_ref[step * block : (step + 1) * block] = (0.5 * jnp.tanh(0.5 * gates) + 0.5).reshape(
            block, cols, channels
        )
    lay_out(pieces, near_ref)
    for wait in waits:
        wait()


def pairs_kernel(near_ref, *refs):
    pieces, lefts, (out_ref, far_scr) = refs[: 2 * GROUPS], refs[2 * GROUPS : 4 * GROUPS], refs[4 * GROUPS :]
    half, parity, wide, _, _ = own_bits()
    share, rows, _ = lefts[0].shape
    lay_out(pieces, far_scr)
    count = 2 * far_scr.shape[2]
    first = lax.broadcasted_iota(jnp.int32, (GROUPS, rows // 2, count), 2) < count // 2
    for pair in range(share // 2):
        packed = []
        for c in (2 * pair, 2 * pair + 1):
            left = jnp.concatenate(
                [jnp.concatenate([lefts[2 * at + q][c] for at in range(GROUPS)], axis=0) for q in range(2)], axis=1
            )
            right = jnp.concatenate(
                [jnp.concatenate([near_ref[q, c], far_scr[q, c]], axis=0) for q in range(2)], axis=1
            )
            summed = lax.dot_general(left, right, NT, preferred_element_type=F32)
            rolled = pltpu.roll(summed, count // 2, 1).reshape(GROUPS, 2, rows // 2, count)
            summed = summed.reshape(GROUPS, 2, rows // 2, count)
            packed.append(
                [
                    jnp.where(first, summed[:, 0], rolled[:, 1]),
                    jnp.where(first, rolled[:, 0], summed[:, 1]),
                ]
            )
        for at in range(GROUPS):
            place = 4 * (parity ^ (at >> 1)) + 2 * (wide ^ (at & 1))
            for q in range(2):
                sums = jnp.concatenate([packed[0][q][at], packed[1][q][at]], axis=0)
                out_ref[place + (half ^ q), pair] = sums.astype(BF16)


def output_kernel(summed_ref, gating_ref, gain_ref, bias_ref, w_ref, out_hbm, scr, out_scr, sems):
    rows, cols, _ = out_scr.shape
    hidden = w_ref.shape[0]
    low = rows // 2
    for part in range(2):
        values = summed_ref[part * GROUPS : (part + 1) * GROUPS].astype(F32).reshape(hidden, low, cols)
        average = jnp.sum(values, axis=0, keepdims=True) / hidden
        centred = values - average
        variance = jnp.sum(jnp.square(centred), axis=0, keepdims=True) / hidden
        scr[part] = (centred * lax.rsqrt(variance + EPSILON)).reshape(hidden * low, cols)
    waits = []
    for row in range(low):
        for part in range(2):
            scaled = scr[part, pl.ds(row, hidden, stride=low), :].T
            normed_sum = (scaled * gain_ref[...] + bias_ref[...]).astype(BF16)
            result = jnp.dot(normed_sum, w_ref[...], preferred_element_type=F32)
            for high in range(2):
                at, where = row + high * low, slice(part * cols // 2, (part + 1) * cols // 2)
                out_scr[at, where] = gating_ref[at, where] * result[high * cols // 2 : (high + 1) * cols // 2]
        if row % 2:
            for high in range(2):
                ready = pl.ds(row - 1 + high * low, 2)
                waits += start_copies(
                    [(out_scr.at[ready], out_hbm.at[ready])], sems.at[pl.ds(row // 2 + high * low // 2, 1)]
                )
    for wait in waits:
        wait()


def exchanged(pair_map, pair_mask, in_gain, in_bias, w_proj, w_gate, out_gain, out_bias, w_out, *, col_parts):
    rows, cols, channels = pair_map.shape
    hidden = w_out.shape[0]
    share = hidden // GROUPS
    half, parity, wide, core, col = [col_parts << bit for bit in reversed(range(ROW_BITS))] + [1]
    plane = [0, col, wide, wide + col]
    devices = range(2 * half)

    def swap(array, offset):
        if not offset:
            return array
        return lax.ppermute(array, ("row", "col"), [(n, n ^ offset) for n in devices])

    params = pltpu.CompilerParams(vmem_limit_bytes=VMEM_LIMIT)
    inputs = (pair_map, pair_mask, in_gain.reshape(1, -1), in_bias.reshape(1, -1), w_proj)
    piece = jax.ShapeDtypeStruct((share, rows, cols), BF16)
    laid_out = jax.ShapeDtypeStruct((2, share, 4 * rows, cols), BF16)
    turned_shape = pltpu.VMEM((2 * hidden, channels), BF16)
    side_shape = pltpu.VMEM((hidden * rows, cols), F32)
    *rights, normed = pl.pallas_call(
        right_kernel,
        in_specs=[HBM] * 5,
        out_specs=[VMEM] * (GROUPS + 1),
        out_shape=[piece] * GROUPS + [jax.ShapeDtypeStruct((rows * cols, channels), BF16)],
        scratch_shapes=[
            pltpu.VMEM((rows, cols, channels), F32),
            pltpu.VMEM((rows, cols), pair_mask.dtype),
            pltpu.VMEM((1, channels), F32),
            pltpu.VMEM((1, channels), F32),
            pltpu.VMEM((channels, 2 * hidden), BF16),
            turned_shape,
            side_shape,
            pltpu.SemaphoreType.DMA((5,)),
        ],
        compiler_params=params,
        name="right",
    )(*[in_hbm(x) for x in inputs])
    lefts = pl.pallas_call(
        left_kernel,
        in_specs=[VMEM] * 3,
        out_specs=[VMEM] * GROUPS,
        out_shape=[piece] * GROUPS,
        scratch_shapes=[turned_shape, side_shape],
        compiler_params=params,
        name="left",
    )(normed, pair_mask, w_proj)
    lefts = [swap(x, plane[n]) for n, x in enumerate(lefts)]
    lefts += [swap(x, parity) for x in lefts]
    rights = [swap(x, plane[n]) for n, x in enumerate(rights)]
    rights += [swap(x, half) for x in rights]
    across = [swap(x, core) for x in rights]
    gating, gain, bias, w_last, near = pl.pallas_call(
        gates_kernel,
        in_specs=[VMEM] * (2 * GROUPS + 2) + [HBM] * 3,
        out_specs=[VMEM] * 5,
        out_shape=[
            jax.ShapeDtypeStruct((rows, cols, channels), F32),
            jax.ShapeDtypeStruct((1, hidden), F32),
            jax.ShapeDtypeStruct((1, hidden), F32),
            jax.ShapeDtypeStruct(w_out.shape, BF16),
            laid_out,
        ],
        scratch_shapes=[pltpu.SemaphoreType.DMA((3,))],
        compiler_params=params,
        name="gates",
    )(
        normed,
        w_gate,
        *rights[:GROUPS],
        *across[:GROUPS],
        in_hbm(out_gain.reshape(1, -1)),
        in_hbm(out_bias.reshape(1, -1)),
        in_hbm(w_out),
    )
    summed = pl.pallas_call(
        pairs_kernel,
        in_specs=[VMEM] * (4 * GROUPS + 1),
        out_specs=VMEM,
        out_shape=jax.ShapeDtypeStruct((2 * GROUPS, share // 2, rows, cols), BF16),
        scratch_shapes=[pltpu.VMEM(laid_out.shape, BF16)],
        compiler_params=params,
        name="pairs",
    )(near, *rights[GROUPS:], *across[GROUPS:], *lefts)
    circles = [
        [own + other + offset for other in (0, parity) for offset in plane]
        for own in (0, core, half, half + core)
    ]
    summed = lax.all_to_all(summed, ("row", "col"), 0, 0, tiled=True, axis_index_groups=circles)
    return pl.pallas_call(
        output_kernel,
        in_specs=[VMEM] * 5,
        out_specs=HBM,
        out_shape=pltpu.MemorySpace.HBM((rows, cols, channels), F32),
        scratch_shapes=[
            pltpu.VMEM((2, hidden * rows // 2, cols), F32),
            pltpu.VMEM((rows, cols, channels), F32),
            pltpu.SemaphoreType.DMA((rows // 2,)),
        ],
        compiler_params=params,
        name="output",
    )(summed, gating, gain, bias, w_last)


def solution(mesh):
    row_parts, col_parts = mesh.shape["row"], mesh.shape["col"]

    def local(pair_map, pair_mask, in_gain, in_bias, w_proj, w_gate, out_gain, out_bias, w_out):
        rows, cols, channels = pair_map.shape
        hidden = w_out.shape[0]
        whole_tiles = rows % 16 == 0 and cols % 128 == 0 and channels % 128 == 0 and hidden % 128 == 0
        bits = row_parts == 2**ROW_BITS and col_parts == 2 and rows * row_parts == col_parts * cols
        plan = gathered
        if whole_tiles and bits:
            plan = functools.partial(exchanged, col_parts=col_parts)
        return plan(pair_map, pair_mask, in_gain, in_bias, w_proj, w_gate, out_gain, out_bias, w_out)

    in_specs = (P("row", "col", None), P("row", "col"), P(), P(), P(), P(), P(), P(), P())
    out_specs = P("row", "col", None)
    return jax.shard_map(local, mesh=mesh, in_specs=in_specs, out_specs=out_specs, check_vma=False)
```

```python
import functools

import jax
import jax.numpy as jnp
from jax import lax
from jax.experimental import pallas as pl
from jax.experimental.pallas import tpu as pltpu
from jax.sharding import PartitionSpec as P


F32 = jnp.float32
BF16 = jnp.bfloat16
EPSILON = 1e-05
NT = (((1,), (1,)), ((), ()))


def layer_norm(values, gain, bias):
    average = jnp.mean(values, axis=-1, keepdims=True)
    variance = jnp.mean(jnp.square(values - average), axis=-1, keepdims=True)
    return (values - average) * lax.rsqrt(variance + EPSILON) * gain + bias


def gathered(pair_map, pair_mask, in_gain, in_bias, w_proj, w_gate, out_gain, out_bias, w_out):
    row_count, col_count, channels = pair_map.shape
    hidden_width = w_out.shape[0]
    normed_map = layer_norm(pair_map, in_gain, in_bias).astype(BF16)
    flattened = normed_map.reshape(-1, channels)
    projected_all = jnp.dot(flattened, w_proj, preferred_element_type=F32).reshape(
        row_count, col_count, 4 * hidden_width
    )
    masked = pair_mask.astype(F32)[..., None]
    left_side = (
        masked
        * jax.nn.sigmoid(projected_all[..., :hidden_width])
        * projected_all[..., hidden_width : 2 * hidden_width]
    ).astype(BF16)
    gating = jax.nn.sigmoid(jnp.dot(flattened, w_gate, preferred_element_type=F32)).reshape(
        row_count, col_count, channels
    )
    right_side = (
        masked
        * jax.nn.sigmoid(projected_all[..., 2 * hidden_width : 3 * hidden_width])
        * projected_all[..., 3 * hidden_width :]
    ).astype(BF16)
    partial_value = jnp.einsum(
        "ikc,jkc->ijc",
        left_side,
        lax.all_gather(right_side, "row", axis=0, tiled=True),
        preferred_element_type=F32,
    )
    summed = lax.psum_scatter(partial_value, "col", scatter_dimension=1, tiled=True)
    normed_sum = layer_norm(summed, out_gain, out_bias).astype(BF16)
    result = jnp.dot(normed_sum.reshape(-1, hidden_width), w_out, preferred_element_type=F32).reshape(
        row_count, col_count, channels
    )
    return gating * result


ROW_BITS = 4
GROUPS = 4
VMEM_LIMIT = 16 * 2**20
HBM = pl.BlockSpec(memory_space=pltpu.MemorySpace.HBM)
VMEM = pl.BlockSpec(memory_space=pltpu.MemorySpace.VMEM)


def gated(half_gate, half_value):
    return half_value * jnp.tanh(half_gate) + half_value


def in_hbm(array):
    return pltpu.with_memory_space_constraint(array, pltpu.MemorySpace.HBM)


def own_bits():
    row, col = lax.axis_index("row"), lax.axis_index("col")
    return [(row >> bit) & 1 for bit in reversed(range(ROW_BITS))] + [col]


def start_copies(pairs, semaphores):
    copies = [pltpu.make_async_copy(source, target, semaphores.at[n]) for n, (source, target) in enumerate(pairs)]
    for copy in copies:
        copy.start()
    return [copy.wait for copy in copies]


def turn(w_ref, w_turned):
    hidden = w_ref.shape[1] // 2
    for part, scale in enumerate((0.5, 1.0)):
        columns = w_ref[:, part * hidden : (part + 1) * hidden].astype(F32)
        w_turned[part * hidden : (part + 1) * hidden, :] = (scale * columns).T.astype(BF16)


def project(normed, w_turned, mask_ref, side_scr, first):
    rows, cols = mask_ref.shape
    hidden = w_turned.shape[0] // 2
    projected = lax.dot_general(w_turned[...], normed, NT, preferred_element_type=F32)
    for at in range(normed.shape[0] // cols):
        row = first + at
        here = projected[:, at * cols : (at + 1) * cols]
        half_masked = 0.5 * mask_ref[row : row + 1, :].astype(F32)
        side_scr[pl.ds(row, hidden, stride=rows), :] = gated(here[:hidden], half_masked * here[hidden:])


def cut(side_scr, outs):
    _, _, wide, _, col = own_bits()
    share, rows, cols = outs[0].shape
    for offset, out_ref in enumerate(outs):
        start = pl.multiple_of(((2 * wide + col) ^ offset) * (share * rows), share * rows)
        out_ref[...] = side_scr[pl.ds(start, share * rows), :].astype(BF16).reshape(share, rows, cols)


def right_kernel(map_hbm, mask_hbm, gain_hbm, bias_hbm, w_hbm, *refs):
    outs, normed_ref = refs[:GROUPS], refs[GROUPS]
    map_scr, mask_scr, gain_scr, bias_scr, w_scr, w_turned, side_scr, sems = refs[GROUPS + 1 :]
    rows, cols, channels = map_scr.shape
    width = w_scr.shape[1]
    wait_map, wait_w, wait_gain, wait_bias, wait_mask = start_copies(
        [
            (map_hbm, map_scr),
            (w_hbm.at[:, width : 2 * width], w_scr),
            (gain_hbm, gain_scr),
            (bias_hbm, bias_scr),
            (mask_hbm, mask_scr),
        ],
        sems,
    )
    wait_w()
    turn(w_scr, w_turned)
    wait_gain()
    wait_bias()
    wait_mask()
    wait_map()
    block = rows // 8
    for step in range(8):
        values = map_scr[step * block : (step + 1) * block].reshape(block * cols, channels)
        normed = layer_norm(values, gain_scr[...], bias_scr[...]).astype(BF16)
        normed_ref[step * block * cols : (step + 1) * block * cols, :] = normed
        project(normed, w_turned, mask_scr, side_scr, step * block)
    cut(side_scr, outs)


def left_kernel(normed_ref, mask_ref, w_ref, *refs):
    outs, (w_turned, side_scr) = refs[:GROUPS], refs[GROUPS:]
    rows, cols = mask_ref.shape
    turn(w_ref.at[:, : w_ref.shape[1] // 2], w_turned)
    block = rows // 4
    for step in range(4):
        normed = normed_ref[step * block * cols : (step + 1) * block * cols, :]
        project(normed, w_turned, mask_ref, side_scr, step * block)
    cut(side_scr, outs)


def lay_out(pieces, out_ref):
    _, _, wide, core, _ = own_bits()
    rows = pieces[0].shape[1]
    for n, piece in enumerate(pieces):
        block = 2 * (wide ^ ((n >> 1) & 1)) + (core ^ (n >> 2))
        out_ref[n & 1, :, pl.ds(pl.multiple_of(block * rows, rows), rows), :] = piece[...]


def gates_kernel(normed_ref, w_gate_ref, *refs):
    pieces, (gain_hbm, bias_hbm, w_out_hbm) = refs[: 2 * GROUPS], refs[2 * GROUPS : 2 * GROUPS + 3]
    gating_ref, gain_ref, bias_ref, w_out_ref, near_ref, sems = refs[2 * GROUPS + 3 :]
    waits = start_copies([(gain_hbm, gain_ref), (bias_hbm, bias_ref), (w_out_hbm, w_out_ref)], sems)
    rows, cols, channels = gating_ref.shape
    block = rows // 4
    for step in range(4):
        normed = normed_ref[step * block * cols : (step + 1) * block * cols, :]
        gates = jnp.dot(normed, w_gate_ref[...], preferred_element_type=F32)
        gating_ref[step * block : (step + 1) * block] = (0.5 * jnp.tanh(0.5 * gates) + 0.5).reshape(
            block, cols, channels
        )
    lay_out(pieces, near_ref)
    for wait in waits:
        wait()


def pairs_kernel(near_ref, *refs):
    pieces, lefts, (out_ref, far_scr) = refs[: 2 * GROUPS], refs[2 * GROUPS : 4 * GROUPS], refs[4 * GROUPS :]
    half, parity, wide, _, _ = own_bits()
    share, rows, _ = lefts[0].shape
    lay_out(pieces, far_scr)
    count = 2 * far_scr.shape[2]
    first = lax.broadcasted_iota(jnp.int32, (GROUPS, rows // 2, count), 2) < count // 2
    for pair in range(share // 2):
        packed = []
        for c in (2 * pair, 2 * pair + 1):
            left = jnp.concatenate(
                [jnp.concatenate([lefts[2 * at + q][c] for at in range(GROUPS)], axis=0) for q in range(2)], axis=1
            )
            right = jnp.concatenate(
                [jnp.concatenate([near_ref[q, c], far_scr[q, c]], axis=0) for q in range(2)], axis=1
            )
            summed = lax.dot_general(left, right, NT, preferred_element_type=F32)
            rolled = pltpu.roll(summed, count // 2, 1).reshape(GROUPS, 2, rows // 2, count)
            summed = summed.reshape(GROUPS, 2, rows // 2, count)
            packed.append(
                [
                    jnp.where(first, summed[:, 0], rolled[:, 1]),
                    jnp.where(first, rolled[:, 0], summed[:, 1]),
                ]
            )
        for at in range(GROUPS):
            place = 4 * (parity ^ (at >> 1)) + 2 * (wide ^ (at & 1))
            for q in range(2):
                sums = jnp.concatenate([packed[0][q][at], packed[1][q][at]], axis=0)
                out_ref[place + (half ^ q), pair] = sums.astype(BF16)


def output_kernel(summed_ref, gating_ref, gain_ref, bias_ref, w_ref, out_hbm, scr, out_scr, sems):
    rows, cols, _ = out_scr.shape
    hidden = w_ref.shape[0]
    low = rows // 2
    for part in range(2):
        values = summed_ref[part * GROUPS : (part + 1) * GROUPS].astype(F32).reshape(hidden, low, cols)
        average = jnp.sum(values, axis=0, keepdims=True) / hidden
        centred = values - average
        variance = jnp.sum(jnp.square(centred), axis=0, keepdims=True) / hidden
        scr[part] = (centred * lax.rsqrt(variance + EPSILON)).reshape(hidden * low, cols)
    waits = []
    for row in range(low):
        for part in range(2):
            scaled = scr[part, pl.ds(row, hidden, stride=low), :].T
            normed_sum = (scaled * gain_ref[...] + bias_ref[...]).astype(BF16)
            result = jnp.dot(normed_sum, w_ref[...], preferred_element_type=F32)
            for high in range(2):
                at, where = row + high * low, slice(part * cols // 2, (part + 1) * cols // 2)
                out_scr[at, where] = gating_ref[at, where] * result[high * cols // 2 : (high + 1) * cols // 2]
        for high in range(2):
            ready = pl.ds(row + high * low, 1)
            waits += start_copies([(out_scr.at[ready], out_hbm.at[ready])], sems.at[ready])
    for wait in waits:
        wait()


def exchanged(pair_map, pair_mask, in_gain, in_bias, w_proj, w_gate, out_gain, out_bias, w_out, *, col_parts):
    rows, cols, channels = pair_map.shape
    hidden = w_out.shape[0]
    share = hidden // GROUPS
    half, parity, wide, core, col = [col_parts << bit for bit in reversed(range(ROW_BITS))] + [1]
    plane = [0, col, wide, wide + col]
    devices = range(2 * half)

    def swap(array, offset):
        if not offset:
            return array
        return lax.ppermute(array, ("row", "col"), [(n, n ^ offset) for n in devices])

    params = pltpu.CompilerParams(vmem_limit_bytes=VMEM_LIMIT)
    inputs = (pair_map, pair_mask, in_gain.reshape(1, -1), in_bias.reshape(1, -1), w_proj)
    piece = jax.ShapeDtypeStruct((share, rows, cols), BF16)
    laid_out = jax.ShapeDtypeStruct((2, share, 4 * rows, cols), BF16)
    turned_shape = pltpu.VMEM((2 * hidden, channels), BF16)
    side_shape = pltpu.VMEM((hidden * rows, cols), F32)
    *rights, normed = pl.pallas_call(
        right_kernel,
        in_specs=[HBM] * 5,
        out_specs=[VMEM] * (GROUPS + 1),
        out_shape=[piece] * GROUPS + [jax.ShapeDtypeStruct((rows * cols, channels), BF16)],
        scratch_shapes=[
            pltpu.VMEM((rows, cols, channels), F32),
            pltpu.VMEM((rows, cols), pair_mask.dtype),
            pltpu.VMEM((1, channels), F32),
            pltpu.VMEM((1, channels), F32),
            pltpu.VMEM((channels, 2 * hidden), BF16),
            turned_shape,
            side_shape,
            pltpu.SemaphoreType.DMA((5,)),
        ],
        compiler_params=params,
        name="right",
    )(*[in_hbm(x) for x in inputs])
    lefts = pl.pallas_call(
        left_kernel,
        in_specs=[VMEM] * 3,
        out_specs=[VMEM] * GROUPS,
        out_shape=[piece] * GROUPS,
        scratch_shapes=[turned_shape, side_shape],
        compiler_params=params,
        name="left",
    )(normed, pair_mask, w_proj)
    lefts = [swap(x, plane[n]) for n, x in enumerate(lefts)]
    lefts += [swap(x, parity) for x in lefts]
    rights = [swap(x, plane[n]) for n, x in enumerate(rights)]
    rights += [swap(x, half) for x in rights]
    across = [swap(x, core) for x in rights]
    gating, gain, bias, w_last, near = pl.pallas_call(
        gates_kernel,
        in_specs=[VMEM] * (2 * GROUPS + 2) + [HBM] * 3,
        out_specs=[VMEM] * 5,
        out_shape=[
            jax.ShapeDtypeStruct((rows, cols, channels), F32),
            jax.ShapeDtypeStruct((1, hidden), F32),
            jax.ShapeDtypeStruct((1, hidden), F32),
            jax.ShapeDtypeStruct(w_out.shape, BF16),
            laid_out,
        ],
        scratch_shapes=[pltpu.SemaphoreType.DMA((3,))],
        compiler_params=params,
        name="gates",
    )(
        normed,
        w_gate,
        *rights[:GROUPS],
        *across[:GROUPS],
        in_hbm(out_gain.reshape(1, -1)),
        in_hbm(out_bias.reshape(1, -1)),
        in_hbm(w_out),
    )
    summed = pl.pallas_call(
        pairs_kernel,
        in_specs=[VMEM] * (4 * GROUPS + 1),
        out_specs=VMEM,
        out_shape=jax.ShapeDtypeStruct((2 * GROUPS, share // 2, rows, cols), BF16),
        scratch_shapes=[pltpu.VMEM(laid_out.shape, BF16)],
        compiler_params=params,
        name="pairs",
    )(near, *rights[GROUPS:], *across[GROUPS:], *lefts)
    circles = [
        [own + other + offset for other in (0, parity) for offset in plane]
        for own in (0, core, half, half + core)
    ]
    summed = lax.all_to_all(summed, ("row", "col"), 0, 0, tiled=True, axis_index_groups=circles)
    return pl.pallas_call(
        output_kernel,
        in_specs=[VMEM] * 5,
        out_specs=HBM,
        out_shape=pltpu.MemorySpace.HBM((rows, cols, channels), F32),
        scratch_shapes=[
            pltpu.VMEM((2, hidden * rows // 2, cols), F32),
            pltpu.VMEM((rows, cols, channels), F32),
            pltpu.SemaphoreType.DMA((rows,)),
        ],
        compiler_params=params,
        name="output",
    )(summed, gating, gain, bias, w_last)


def solution(mesh):
    row_parts, col_parts = mesh.shape["row"], mesh.shape["col"]

    def local(pair_map, pair_mask, in_gain, in_bias, w_proj, w_gate, out_gain, out_bias, w_out):
        rows, cols, channels = pair_map.shape
        hidden = w_out.shape[0]
        whole_tiles = rows % 16 == 0 and cols % 128 == 0 and channels % 128 == 0 and hidden % 128 == 0
        bits = row_parts == 2**ROW_BITS and col_parts == 2 and rows * row_parts == col_parts * cols
        plan = gathered
        if whole_tiles and bits:
            plan = functools.partial(exchanged, col_parts=col_parts)
        return plan(pair_map, pair_mask, in_gain, in_bias, w_proj, w_gate, out_gain, out_bias, w_out)

    in_specs = (P("row", "col", None), P("row", "col"), P(), P(), P(), P(), P(), P(), P())
    out_specs = P("row", "col", None)
    return jax.shard_map(local, mesh=mesh, in_specs=in_specs, out_specs=out_specs, check_vma=False)
```
